32 devices in a mesh: gx: 4 (over z), gy: 4 (over y, x), gz: 2 (over core).
Axes of the slice: x: 2, y: 2, z: 4, core: 2. Of those that a mesh axis runs over, the one named last changes fastest.
Arguments:
- eigvecs: bfloat16 [64, 32, 96, 512], P('gx', 'gy', 'gz'), may hold values from -7 to 7, as said below
- material: float32 [2, 64, 32, 96], P(None, 'gx', 'gy', 'gz'), may hold values from 0.5 to 2
Outputs:
- stiffness: float32 [512, 512], P(('gx', 'gy', 'gz'))
- mass_matrix: float32 [512, 512], P(('gx', 'gy', 'gz'))
The draws below stay inside these ranges and needn't reach their ends.
Inputs may be any that keep to these rules, and one draw needn't show every extreme that they name: `eigvecs`: entries are a rough part plus a part that varies slowly over the grid.
All inputs are finite; a program needn't handle non-finite values.
Results may differ from the reference program's by a relative error of at most 0.0003.
Values may be sent and summed in bfloat16 or wider, within the bound.
A program may use at most 128 MiB of HBM per device.

```python
import math
import jax
import jax.numpy as jnp
from jax import lax

K = 512
NX = 64
NY = 32
NZ = 96


def draw_eigvecs(key, part):
    keys = jax.random.split(key, 7)
    rough = jnp.clip(jax.random.normal(keys[0], (NX, NY, NZ, K), jnp.float32), -4.0, 4.0)
    amplitude = 2.0
    freq_x = jax.random.randint(keys[1], (K,), 1, 4).astype(jnp.float32)
    freq_y = jax.random.randint(keys[2], (K,), 1, 4).astype(jnp.float32)
    freq_z = jax.random.randint(keys[3], (K,), 1, 4).astype(jnp.float32)
    phase_x = jax.random.uniform(keys[4], (K,), jnp.float32)
    phase_y = jax.random.uniform(keys[5], (K,), jnp.float32)
    phase_z = jax.random.uniform(keys[6], (K,), jnp.float32)
    coord_x = jnp.arange(NX, dtype=jnp.float32)[:, None] / NX
    coord_y = jnp.arange(NY, dtype=jnp.float32)[:, None] / NY
    coord_z = jnp.arange(NZ, dtype=jnp.float32)[:, None] / NZ
    wave_x = jnp.cos(2.0 * jnp.pi * (coord_x * freq_x + phase_x))
    wave_y = jnp.cos(2.0 * jnp.pi * (coord_y * freq_y + phase_y))
    wave_z = jnp.cos(2.0 * jnp.pi * (coord_z * freq_z + phase_z))
    smooth = wave_x[:, None, None, :] * wave_y[None, :, None, :] * wave_z[None, None, :, :]
    return (rough + amplitude * smooth).astype(jnp.bfloat16)


def shard_levels(own_key, shape, cuts, low, top_value):
    factor_of = 1.0
    for dim, shards_of in cuts:
        heights = jax.random.uniform(jax.random.fold_in(jax.random.fold_in(own_key, 6), dim), (shards_of,), jnp.float32, low / len(cuts), top_value / len(cuts))
        factor_of = factor_of * jnp.repeat(jnp.exp(heights), shape[dim] // shards_of).reshape((-1,) + (1,) * (len(shape) - 1 - dim))
    return factor_of


def setup_inputs(seed: int = 0) -> dict:
    streams_of = jax.random.split(jax.random.key(seed), 3)
    eigvecs = draw_eigvecs(jax.random.fold_in(streams_of[2], 71), 0)
    material = jnp.clip(jnp.exp(math.log(2.0) - 1.3862944 * jax.random.uniform(streams_of[1], (2, NX, NY, NZ), jnp.float32) ** shard_levels(streams_of[1], (2, NX, NY, NZ), ((1, 4), (2, 4), (3, 2)), -0.2, 0.2)), 0.5, 2.0)
    return {"eigvecs": eigvecs, "material": material}


stencil_offsets = [(dx, dy, dz) for dx in (-1, 0, 1) for dy in (-1, 0, 1) for dz in (-1, 0, 1) if (dx, dy, dz) != (0, 0, 0)]


def coupling(offset):
    nonzero = sum(abs(entry) for entry in offset)
    return 0.25 * 0.5 ** (nonzero - 1)


def mass_weight(offset):
    weight = 1.0
    for entry in offset:
        weight = weight * (4.0 / 6.0 if entry == 0 else 1.0 / 6.0)
    return weight


def apply_operators(padded, padded_material):
    size_x = padded.shape[0] - 2
    size_y = padded.shape[1] - 2
    size_z = padded.shape[2] - 2
    centre = padded[1:-1, 1:-1, 1:-1].astype(jnp.float32)
    kappa_centre = padded_material[0, 1:-1, 1:-1, 1:-1]
    rho_centre = padded_material[1, 1:-1, 1:-1, 1:-1]
    stiff_sum = jnp.zeros(centre.shape, jnp.float32)
    mass_sum = mass_weight((0, 0, 0)) * rho_centre[..., None] * centre
    for offset in stencil_offsets:
        lower = (1 + offset[0], 1 + offset[1], 1 + offset[2])
        shifted = padded[lower[0]:lower[0] + size_x, lower[1]:lower[1] + size_y, lower[2]:lower[2] + size_z].astype(jnp.float32)
        kappa_side = padded_material[0, lower[0]:lower[0] + size_x, lower[1]:lower[1] + size_y, lower[2]:lower[2] + size_z]
        rho_side = padded_material[1, lower[0]:lower[0] + size_x, lower[1]:lower[1] + size_y, lower[2]:lower[2] + size_z]
        stiff_sum = stiff_sum + (coupling(offset) * 0.5 * (kappa_centre + kappa_side))[..., None] * (centre - shifted)
        mass_sum = mass_sum + (mass_weight(offset) * 0.5 * (rho_centre + rho_side))[..., None] * shifted
    return stiff_sum.astype(jnp.bfloat16), mass_sum.astype(jnp.bfloat16)


def reference(eigvecs, material):
    cells = NX * NY * NZ
    block_cols = 32
    padded_material = jnp.pad(material, ((0, 0), (1, 1), (1, 1), (1, 1)))
    flat_vectors = eigvecs.reshape(cells, K)

    def column_block(block_index):
        first_col = block_index * block_cols
        col_block = lax.dynamic_slice_in_dim(eigvecs, first_col, block_cols, 3)
        padded = jnp.pad(col_block, ((1, 1), (1, 1), (1, 1), (0, 0)))
        stiff_vecs, mass_vecs = apply_operators(padded, padded_material)
        dims = (((0,), (0,)), ((), ()))
        stiff_cols = lax.dot_general(flat_vectors, stiff_vecs.reshape(cells, block_cols), dims, preferred_element_type=jnp.float32)
        mass_cols = lax.dot_general(flat_vectors, mass_vecs.reshape(cells, block_cols), dims, preferred_element_type=jnp.float32)
        return stiff_cols, mass_cols

    stiff_blocks, mass_blocks = lax.map(column_block, jnp.arange(K // block_cols, dtype=jnp.int32))
    stiffness = jnp.transpose(stiff_blocks, (1, 0, 2)).reshape(K, K) / cells
    mass_matrix = jnp.transpose(mass_blocks, (1, 0, 2)).reshape(K, K) / cells
    return stiffness, mass_matrix
```

```python
import functools
import numpy as np
import jax
import jax.numpy as jnp
from jax import lax
from jax.experimental import pallas as pl
from jax.experimental.pallas import tpu as pltpu
from jax.sharding import PartitionSpec as P

LANES = 128
GHOST = 16
MESH = pl.DeviceIdType.MESH


def tap(a, b, middle):
    return middle if a == b else (1.0 if abs(a - b) == 1 else 0.0)


def tap_matrices(size_y, size_z):
    half = size_y // 2
    width = (half + 1) * size_z + GHOST
    sides = []
    for side in (0, 1):
        edge = size_z - 1 if side == 0 else 0
        blocks = []
        for first in (0, 1):
            ys_in = range(0, half + 1) if first == 0 else range(half - 1, size_y)
            ys_out = range(0, half) if first == 0 else range(half, size_y)
            own_at = GHOST if first == 0 else 0
            ghost_at = 0 if first == 0 else (half + 1) * size_z
            rows = []
            for middle in (2.0, 4.0):
                zz = middle * np.eye(size_z) + np.eye(size_z, k=1) + np.eye(size_z, k=-1)
                block = np.zeros((half * size_z, width))
                for o, y in enumerate(ys_out):
                    for n, y2 in enumerate(ys_in):
                        w = tap(y, y2, middle)
                        if w:
                            block[o * size_z:(o + 1) * size_z,
                                  own_at + n * size_z:own_at + (n + 1) * size_z] = w * zz
                            block[o * size_z + edge, ghost_at + y2] = w
                rows.append(block)
            blocks.append(np.concatenate(rows, 0))
        group = size_z + GHOST
        rows = []
        for middle in (2.0, 4.0):
            zz = middle * np.eye(size_z) + np.eye(size_z, k=1) + np.eye(size_z, k=-1)
            one = np.zeros((size_z, group))
            one[:, :size_z] = zz
            one[edge, size_z + (0 if side == 0 else GHOST - 1)] = 1.0
            rows.append(np.kron(np.eye(4), one))
        late = np.concatenate(rows, 0)
        full = np.zeros((blocks[0].shape[0], width))
        full[:late.shape[0], :late.shape[1]] = late
        blocks.append(full)
        sides.append(np.stack(blocks))
    return np.stack(sides)


def kernel(scale, cut, v_ref, mat_ref, t_hbm, stiff_out, mass_out,
           e, p0, p1, p2, p3, ps0, ps1, ya, yb, acc, t, zs, m, mz, fy, cb, gc, g, gk, gr, gg, yl,
           part, rz, sa, sb, ra1, rb1, ta, tb, ra2, rb2, out, local, send, recv):
    f32, bf16 = jnp.float32, jnp.bfloat16
    slots = (p0, p1, p2, p3)
    nx, own, columns = v_ref.shape
    ny_cells, size_z = cb.shape[2:4]
    half = ny_cells // 2
    group = size_z + GHOST
    hz = half * size_z
    kw = t.shape[2]
    gx, gy, gz = (lax.axis_index(a) for a in ("gx", "gy", "gz"))
    cx, cy, cz = (lax.axis_size(a) for a in ("gx", "gy", "gz"))
    has = {("gx", -1): gx > 0, ("gx", 1): gx < cx - 1, ("gy", -1): gy > 0, ("gy", 1): gy < cy - 1}
    at = {"gx": gx, "gy": gy}
    barrier = pltpu.get_barrier_semaphore()
    total = 0
    for axis, count in (("gz", cz), ("gy", cy), ("gx", cx)):
        me = lax.axis_index(axis)
        for k in range(1, count):
            pl.semaphore_signal(barrier, inc=1, device_id={axis: lax.rem(me + k, count)},
                                device_id_type=MESH)
        total += count - 1

    own_v = pltpu.make_async_copy(v_ref, e.at[1:nx + 1, GHOST:GHOST + own], local.at[0])
    own_v.start()
    own_t = pltpu.make_async_copy(t_hbm.at[gz], t, local.at[1])
    own_t.start()

    used = [0]
    sent = []

    def remote(src, dst, device, cond=None, got=None):
        n = used[0]
        used[0] += 1
        copy = pltpu.make_async_remote_copy(src_ref=src, dst_ref=dst, send_sem=send.at[n],
                                            recv_sem=recv.at[n], device_id=device,
                                            device_id_type=MESH)

        def start():
            if cond is None:
                copy.start()
            else:
                pl.when(cond)(copy.start)

        def arrived():
            if got is None:
                copy.wait_recv()
            else:
                pl.when(got)(copy.wait_recv)

        def done():
            if cond is None:
                copy.wait_send()
            else:
                pl.when(cond)(copy.wait_send)

        sent.append(done)
        return start, arrived

    def shift(axis, sign, src, dst):
        return remote(src, dst, {axis: at[axis] + sign}, has[axis, sign], has[axis, -sign])

    def partner(src, dst):
        return remote(src, dst, {"gz": lax.rem(gz + 1, cz)})

    def zero(cond, ref):
        @pl.when(jnp.logical_not(cond))
        def _():
            ref[...] = jnp.zeros(ref.shape, ref.dtype)

    zero(has["gx", -1], e.at[0])
    zero(has["gx", 1], e.at[nx + 1])
    zero(has["gy", -1], m.at[:, 0, 8:8 + nx])
    zero(has["gy", 1], m.at[:, ny_cells + 1, 8:8 + nx])
    zero(has["gx", -1], m.at[:, :, 0:8])
    zero(has["gx", 1], m.at[:, :, 8 + nx:16 + nx])
    m[:, 1:ny_cells + 1, 8:8 + nx] = mat_ref[...]
    g[nx + 2:] = jnp.zeros((g.shape[0] - nx - 2,) + g.shape[1:], bf16)
    top = has["gy", 1]
    zero(top, g.at[1:nx + 1])
    zero(jnp.logical_and(top, has["gx", -1]), g.at[0])
    zero(jnp.logical_and(top, has["gx", 1]), g.at[nx + 1])

    pl.semaphore_wait(barrier, total)

    my_down = shift("gy", -1, mat_ref.at[:, 0], m.at[:, ny_cells + 1, 8:8 + nx])
    my_up = shift("gy", 1, mat_ref.at[:, ny_cells - 1], m.at[:, 0, 8:8 + nx])
    my_down[0]()
    my_up[0]()
    bounds = [(0, 1), (nx - 1, nx)] + [(a, min(a + 4, nx - 1)) for a in range(1, nx - 1, 4)]
    y_ghosts = [shift("gy", -1, v_ref.at[a:b, :size_z], g.at[a + 1:b + 1, :size_z]) for a, b in bounds]
    for copy in y_ghosts:
        copy[0]()
    x_down = shift("gx", -1, v_ref.at[0], e.at[nx + 1, GHOST:GHOST + own])
    x_up = shift("gx", 1, v_ref.at[nx - 1], e.at[0, GHOST:GHOST + own])

    edge = jnp.where(gz == 0, size_z - 1, 0)
    row = lax.broadcasted_iota(jnp.int32, (GHOST, own), 0)
    col = lax.broadcasted_iota(jnp.int32, (GHOST, own), 1)
    pick = jnp.logical_and(row < ny_cells, col == row * size_z + edge)
    pick = jnp.where(pick, 1.0, 0.0).astype(bf16)

    def take_edge(x):
        zs[x] = jnp.dot(pick, e[x, GHOST:GHOST + own], preferred_element_type=f32).astype(bf16)

    own_v.wait()

    def two_edges(i, carry):
        take_edge(2 * i + 1)
        take_edge(2 * i + 2)
        return carry

    lax.fori_loop(0, nx // 2, two_edges, 0)
    tail = GHOST + own
    z_own = [partner(zs.at[1:nx + 1], e.at[1:nx + 1, :GHOST]),
             partner(zs.at[1:nx + 1], e.at[1:nx + 1, tail:])]
    for copy in z_own:
        copy[0]()
    my_down[1]()
    my_up[1]()
    mx_down = shift("gx", -1, m.at[:, :, 8:16], m.at[:, :, 8 + nx:16 + nx])
    mx_up = shift("gx", 1, m.at[:, :, nx:8 + nx], m.at[:, :, 0:8])
    mx_down[0]()
    mx_up[0]()
    x_down[0]()
    x_up[0]()

    own_t.wait()
    for copy in z_own:
        copy[1]()

    def taps_of(x, *dsts):
        first = jnp.dot(t[0], e[x + 1, :kw], preferred_element_type=f32)
        second = jnp.dot(t[1], e[x + 1, tail + GHOST - kw:], preferred_element_type=f32)
        for dst in dsts:
            dst[:2 * hz] = first
            dst[2 * hz:] = second

    taps_of(0, p0, ps0)
    taps_of(1, p1, ps1)
    taps_of(2, p2)
    acc[...] = jnp.zeros_like(acc)
    yb[...] = jnp.zeros_like(yb)

    mx_down[1]()
    mx_up[1]()
    mz_copy = partner(m, mz)
    mz_copy[0]()
    mz_copy[1]()

    lanes = lax.broadcasted_iota(jnp.int32, (m.shape[2], LANES), 1)
    turn = jnp.where(gz == 0, size_z - 1, LANES - size_z + 1)

    def z_sum(y):
        k = m[0, y]
        ghost = jnp.where(lanes == edge, pltpu.roll(mz[0, y], turn, 1), 0.0)
        return pltpu.roll(k, 1, 1) + 2.0 * k + pltpu.roll(k, LANES - 1, 1) + ghost

    def coefficients(y, carry):
        fy[...] = z_sum(y) + 2.0 * z_sum(y + 1) + z_sum(y + 2)
        field = fy[7:7 + nx] + 2.0 * fy[8:8 + nx] + fy[9:9 + nx]
        kappa = m[0, y + 1, 8:8 + nx]
        rho = m[1, y + 1, 8:8 + nx]
        both = jnp.concatenate([2.0 * kappa + field * (1.0 / 32.0), kappa * (1.0 / 16.0),
                                rho * (1.0 / 216.0)], 0)
        cols = both.T[:size_z]
        for c in range(3):
            for x in range(nx):
                n = c * nx + x
                cb[c, x, y] = jnp.broadcast_to(cols[:, n:n + 1], (size_z, LANES))
        return carry

    lax.fori_loop(0, ny_cells, coefficients, 0)

    reach = jnp.where(gz == 0, size_z, GHOST)
    mine = lanes < size_z

    def ghost_columns(f, factor):
        k = m[f, ny_cells + 1]
        return jnp.where(mine, k, pltpu.roll(mz[f, ny_cells + 1], reach, 1)) * factor

    pair = jnp.concatenate([ghost_columns(0, 1.0 / 16.0), ghost_columns(1, 1.0 / 216.0)], 0)
    cols = pair.T[:group]
    for f in range(2):
        for j in range(nx + 2):
            n = f * m.shape[2] + 7 + j
            gc[f, j] = jnp.broadcast_to(cols[:, n:n + 1], (group, LANES))

    wide = 2 * LANES
    dims = (((0,), (0,)), ((), ()))

    def spread(c):
        return jnp.concatenate([c, c], 1)

    def values(x, before, now, after, dst, base):
        for y in range(ny_cells):
            h, yy = divmod(y, half)
            sr = slice(2 * hz * h + size_z * yy, 2 * hz * h + size_z * (yy + 1))
            mr = slice(sr.start + hz, sr.stop + hz)
            rr = slice(base + size_z * y, base + size_z * (y + 1))
            d, kq, rq = (spread(cb[c, x, y]) for c in range(3))
            for at_lane in range(0, columns, wide):
                ll = slice(at_lane, at_lane + wide)
                v = e[x + 1, GHOST + size_z * y:GHOST + size_z * (y + 1), ll].astype(f32)
                s = before[sr, ll] + after[sr, ll] + 2.0 * now[sr, ll]
                w = before[mr, ll] + after[mr, ll] + 4.0 * now[mr, ll]
                dst[rr, ll] = (d * v - kq * s).astype(bf16)
                dst[rr, slice(columns + at_lane, columns + at_lane + wide)] = (rq * w).astype(bf16)

    def gram(first, second, src):
        v = jnp.concatenate([e[first + 1, GHOST:tail], e[second + 1, GHOST:tail]], 0)
        acc[...] += lax.dot_general(v, src[...], dims, preferred_element_type=f32)

    def ring(x):
        return slots[(x + 4) % 4]

    def relay(sign, src, dst):
        return remote(g.at[src, :size_z], g.at[dst, :size_z], {"gx": gx + sign},
                      jnp.logical_and(top, has["gx", sign]), jnp.logical_and(top, has["gx", -sign]))

    relays = [relay(-1, 1, nx + 1), relay(1, nx, 0)]

    z_ghosts = [partner(zs.at[x], e.at[x, at_row:at_row + GHOST])
                for x in (0, nx + 1) for at_row in (0, tail)]
    whole = (nx - 4) // 4

    def four(i, carry):
        @pl.when(i == whole - 1)
        def _():
            x_down[1]()
            x_up[1]()
            take_edge(0)
            take_edge(nx + 1)
            for copy in z_ghosts:
                copy[0]()

        b = 4 * i
        taps_of(b + 3, ring(3))
        values(b + 1, ring(0), ring(1), ring(2), ya, 0)
        gram((b + nx - 1) % nx, b, yb)
        taps_of(b + 4, ring(0))
        values(b + 2, ring(1), ring(2), ring(3), ya, own)
        taps_of(b + 5, ring(1))
        values(b + 3, ring(2), ring(3), ring(0), yb, 0)
        gram(b + 1, b + 2, ya)
        taps_of(b + 6, ring(2))
        values(b + 4, ring(3), ring(0), ring(1), yb, own)
        return carry

    lax.fori_loop(0, whole, four, 0)

    for copy in y_ghosts[:2]:
        copy[1]()
    for copy in relays:
        copy[0]()

    for copy in z_ghosts:
        copy[1]()
    b = 4 * whole
    taps_of(b + 3, ring(3))
    values(b + 1, ring(0), ring(1), ring(2), ya, 0)
    gram(b - 1, b, yb)
    taps_of(b + 4, ring(0))
    values(b + 2, ring(1), ring(2), ring(3), ya, own)
    taps_of(-1, ring(1))
    values(b + 3, ring(2), ring(3), ring(0), yb, 0)
    gram(b + 1, b + 2, ya)
    values(0, ring(1), ps0, ps1, yb, own)
    gram(b + 3, 0, yb)

    zrow = pl.multiple_of(jnp.where(gz == 0, size_z - GHOST, 0), GHOST)
    z_relay = remote(g.at[:nx + 2, pl.ds(zrow, GHOST)], g.at[:nx + 2, size_z:],
                     {"gz": lax.rem(gz + 1, cz)}, top, top)

    for copy in y_ghosts[2:]:
        copy[1]()
    for copy in relays:
        copy[1]()
    z_relay[0]()
    z_relay[1]()

    def weigh(j, carry):
        for at_lane in range(0, columns, LANES):
            ll = slice(at_lane, at_lane + LANES)
            v = g[j, :, ll].astype(f32)
            gk[j, :, ll] = (v * gc[0, j]).astype(bf16)
            gr[j, :, ll] = (v * gc[1, j]).astype(bf16)
        return carry

    gk[nx + 2:] = jnp.zeros((gk.shape[0] - nx - 2,) + gk.shape[1:], bf16)
    gr[nx + 2:] = jnp.zeros((gr.shape[0] - nx - 2,) + gr.shape[1:], bf16)
    lax.fori_loop(0, nx + 2, weigh, 0)
    four_z = 4 * size_z

    def ghost_taps(i, carry):
        at4 = pl.ds(4 * i, 4)

        def load(ref):
            return ref[at4].reshape(4 * group, columns)

        both = jnp.dot(t[2, :, :4 * group], load(g), preferred_element_type=f32)
        gg[0, at4] = both[:four_z].reshape(4, size_z, columns)
        gg[1, at4] = both[four_z:2 * four_z].reshape(4, size_z, columns)
        gg[2, at4] = jnp.dot(t[2, :four_z, :4 * group], load(gk),
                             preferred_element_type=f32).reshape(4, size_z, columns)
        gg[3, at4] = jnp.dot(t[2, four_z:2 * four_z, :4 * group], load(gr),
                             preferred_element_type=f32).reshape(4, size_z, columns)
        return carry

    lax.fori_loop(0, g.shape[0] // 4, ghost_taps, 0)

    def late(x, carry):
        def three(kind, middle, ll):
            return gg[kind, x, :, ll] + gg[kind, x + 2, :, ll] + middle * gg[kind, x + 1, :, ll]

        for at_lane in range(0, columns, LANES):
            ll = slice(at_lane, at_lane + LANES)
            kq, rq = cb[1, x, ny_cells - 1], cb[2, x, ny_cells - 1]
            s = kq * three(0, 2.0, ll) + three(2, 2.0, ll)
            w = rq * three(1, 4.0, ll) + three(3, 4.0, ll)
            yl[x, :, ll] = (-s).astype(bf16)
            yl[x, :, slice(columns + at_lane, columns + at_lane + LANES)] = w.astype(bf16)
        return carry

    lax.fori_loop(0, nx, late, 0)
    last = jnp.concatenate([e[x + 1, tail - size_z:tail] for x in range(nx)], 0)
    acc[...] += lax.dot_general(last, yl[...].reshape(nx * size_z, 2 * columns), dims,
                                preferred_element_type=f32)

    rows = stiff_out.shape[0]
    for side in range(2):
        ll = slice(side * columns, (side + 1) * columns)
        a = acc[:, ll]
        a = (a + a.T) * scale
        for n in range(columns // rows):
            i, rest = divmod(n, cy * cz)
            j, k = divmod(rest, cz)
            part[i, j, k, :, ll] = a[n * rows:(n + 1) * rows]

    def everywhere(axis, piece, landing):
        count = lax.axis_size(axis)
        me = lax.axis_index(axis)
        copies = []
        for k in range(1, count):
            peer = lax.rem(me + k, count)
            copy = remote(piece(peer), landing.at[k - 1], {axis: peer})
            copy[0]()
            copies.append(copy)
        return copies

    def collect(copies, held, landing):
        for copy in copies:
            copy[1]()
        for k in range(len(copies)):
            held = held + landing[k]
        return held

    first = everywhere("gz", lambda p: part.at[:, :, p], rz)
    held = collect(first, part[:, :, gz], rz)
    sa[...] = held[..., :cut]
    sb[...] = held[..., cut:]
    a1 = everywhere("gy", lambda p: sa.at[:, p], ra1)
    b1 = everywhere("gx", lambda p: sb.at[p], rb1)
    ta[...] = collect(a1, sa[:, gy], ra1)
    a2 = everywhere("gx", lambda p: ta.at[p], ra2)
    tb[...] = collect(b1, sb[gx], rb1)
    b2 = everywhere("gy", lambda p: tb.at[p], rb2)
    out[:, :cut] = collect(a2, ta[gx], ra2)
    out[:, cut:] = collect(b2, tb[gy], rb2)
    stiff_out[...] = out[:, :columns]
    mass_out[...] = out[:, columns:]
    for done in sent:
        done()


def per_device(eigvecs, material):
    size_x, size_y, size_z, columns = eigvecs.shape
    nx, ny, nz = (lax.axis_size(a) for a in ("gx", "gy", "gz"))
    total_cells = size_x * size_y * size_z * nx * ny * nz
    own = size_y * size_z
    tail = own + 2 * GHOST
    group = size_z + GHOST
    rows = columns // (nx * ny * nz)
    wide = 2 * columns
    cut = (wide * 5 // 8) // LANES * LANES
    rest = wide - cut
    matrices = jnp.asarray(tap_matrices(size_y, size_z), jnp.bfloat16)
    mat = jnp.pad(jnp.transpose(material, (0, 2, 1, 3)),
                  ((0, 0), (0, 0), (0, 0), (0, LANES - size_z)))
    f32, bf16 = jnp.float32, jnp.bfloat16
    dma = pltpu.SemaphoreType.DMA
    vmem = pl.BlockSpec(memory_space=pltpu.VMEM)
    anywhere = pl.BlockSpec(memory_space=pl.ANY)
    late_planes = -(-(size_x + 2) // 4) * 4
    copies = 64 + (nz - 1) + 2 * (nx - 1) + 2 * (ny - 1)
    scratch = [
        ((size_x + 2, tail, columns), bf16),
        ((2 * own, columns), f32), ((2 * own, columns), f32),
        ((2 * own, columns), f32), ((2 * own, columns), f32),
        ((2 * own, columns), f32), ((2 * own, columns), f32),
        ((2 * own, wide), bf16), ((2 * own, wide), bf16),
        ((columns, wide), f32),
        (matrices.shape[1:], bf16),
        ((size_x + 2, GHOST, columns), bf16),
        ((2, size_y + 2, size_x + 16, LANES), f32),
        ((2, size_y + 2, size_x + 16, LANES), f32),
        ((size_x + 16, LANES), f32),
        ((3, size_x, size_y, size_z, LANES), f32),
        ((2, size_x + 2, group, LANES), f32),
        ((late_planes, group, columns), bf16),
        ((late_planes, group, columns), bf16),
        ((late_planes, group, columns), bf16),
        ((4, late_planes, size_z, columns), f32),
        ((size_x, size_z, wide), bf16),
        ((nx, ny, nz, rows, wide), f32),
        ((nz - 1, nx, ny, rows, wide), f32),
        ((nx, ny, rows, cut), f32),
        ((nx, ny, rows, rest), f32),
        ((ny - 1, nx, rows, cut), f32),
        ((nx - 1, ny, rows, rest), f32),
        ((nx, rows, cut), f32),
        ((ny, rows, rest), f32),
        ((nx - 1, rows, cut), f32),
        ((ny - 1, rows, rest), f32),
        ((rows, wide), f32),
    ]
    out = pl.pallas_call(
        functools.partial(kernel, 0.5 / total_cells, cut),
        out_shape=[jax.ShapeDtypeStruct((rows, columns), f32)] * 2,
        in_specs=[anywhere, vmem, anywhere],
        out_specs=[vmem, vmem],
        scratch_shapes=[pltpu.VMEM(*s) for s in scratch] + [dma((2,)), dma((copies,)), dma((copies,))],
        compiler_params=pltpu.CompilerParams(
            vmem_limit_bytes=63 * 1024 * 1024, collective_id=0, has_side_effects=True),
    )(eigvecs.reshape(size_x, own, columns), mat, matrices)
    return tuple(out)


def solution(mesh):
    return jax.shard_map(
        per_device,
        mesh=mesh,
        in_specs=(P("gx", "gy", "gz", None), P(None, "gx", "gy", "gz")),
        out_specs=(P(("gx", "gy", "gz"), None), P(("gx", "gy", "gz"), None)),
        check_vma=False,
    )
```

```python
import functools
import numpy as np
import jax
import jax.numpy as jnp
from jax import lax
from jax.experimental import pallas as pl
from jax.experimental.pallas import tpu as pltpu
from jax.sharding import PartitionSpec as P

LANES = 128
GHOST = 16
MESH = pl.DeviceIdType.MESH
AXES = ("gx", "gy", "gz")


def tap(a, b, middle):
    return middle if a == b else (1.0 if abs(a - b) == 1 else 0.0)


def tap_matrices(size_y, size_z):
    half = size_y // 2
    width = (half + 1) * size_z + GHOST
    sides = []
    for side in (0, 1):
        edge = size_z - 1 if side == 0 else 0
        blocks = []
        for first in (0, 1):
            ys_in = range(0, half + 1) if first == 0 else range(half - 1, size_y)
            ys_out = range(0, half) if first == 0 else range(half, size_y)
            own_at = GHOST if first == 0 else 0
            ghost_at = 0 if first == 0 else (half + 1) * size_z
            rows = []
            for middle in (2.0, 4.0):
                zz = middle * np.eye(size_z) + np.eye(size_z, k=1) + np.eye(size_z, k=-1)
                block = np.zeros((half * size_z, width))
                for o, y in enumerate(ys_out):
                    for n, y2 in enumerate(ys_in):
                        w = tap(y, y2, middle)
                        if w:
                            block[o * size_z:(o + 1) * size_z,
                                  own_at + n * size_z:own_at + (n + 1) * size_z] = w * zz
                            block[o * size_z + edge, ghost_at + y2] = w
                rows.append(block)
            blocks.append(np.concatenate(rows, 0))
        group = size_z + GHOST
        rows = []
        for middle in (2.0, 4.0):
            zz = middle * np.eye(size_z) + np.eye(size_z, k=1) + np.eye(size_z, k=-1)
            one = np.zeros((size_z, group))
            one[:, :size_z] = zz
            one[edge, size_z + (0 if side == 0 else GHOST - 1)] = 1.0
            rows.append(np.kron(np.eye(4), one))
        late = np.concatenate(rows, 0)
        full = np.zeros((blocks[0].shape[0], width))
        full[:late.shape[0], :late.shape[1]] = late
        blocks.append(full)
        sides.append(np.stack(blocks))
    return np.stack(sides)


def kernel(scale, chunks, v_ref, mat_ref, t_hbm, out_ref,
           e, pp, ps0, ps1, ya, yb, acc, t, zs, cz_out, cz_in, m, mz, fy, cols, gc, g, gk, gr, gg, yl,
           part, *rest):
    f32, bf16 = jnp.float32, jnp.bfloat16
    local, send, recv = rest[-3:]
    buffers = [rest[5 * n:5 * n + 5] for n in range(len(chunks))]
    nx, own, columns = v_ref.shape
    ny_cells, size_z = mat_ref.shape[2:]
    half = ny_cells // 2
    group = size_z + GHOST
    hz = half * size_z
    kw = t.shape[2]
    tail = GHOST + own
    gx, gy, gz = (lax.axis_index(a) for a in AXES)
    cx, cy, cz = (lax.axis_size(a) for a in AXES)
    has = {("gx", -1): gx > 0, ("gx", 1): gx < cx - 1, ("gy", -1): gy > 0, ("gy", 1): gy < cy - 1}
    at = {"gx": gx, "gy": gy}
    top = has["gy", 1]
    other = lax.rem(gz + 1, cz)
    barrier = pltpu.get_barrier_semaphore()
    total = 0
    for axis, count in (("gz", cz), ("gy", cy), ("gx", cx)):
        me = lax.axis_index(axis)
        for k in range(1, count):
            pl.semaphore_signal(barrier, inc=1, device_id={axis: lax.rem(me + k, count)},
                                device_id_type=MESH)
        total += count - 1
    for sign in (-1, 1):
        @pl.when(has["gy", sign])
        def _(sign=sign):
            pl.semaphore_signal(barrier, inc=1, device_id={"gy": gy + sign, "gz": other},
                                device_id_type=MESH)
        total = total + jnp.where(has["gy", sign], 1, 0)

    own_v = pltpu.make_async_copy(v_ref, e.at[1:nx + 1, GHOST:tail], local.at[0])
    own_v.start()
    own_t = pltpu.make_async_copy(t_hbm.at[gz], t, local.at[1])
    own_t.start()

    used = [0]
    sent = []

    def remote(src, dst, device, cond=None, got=None):
        n = used[0]
        used[0] += 1
        copy = pltpu.make_async_remote_copy(src_ref=src, dst_ref=dst, send_sem=send.at[n],
                                            recv_sem=recv.at[n], device_id=device,
                                            device_id_type=MESH)

        def when(test, action):
            if test is None:
                action()
            else:
                pl.when(test)(action)

        sent.append(lambda: when(cond, copy.wait_send))
        return lambda: when(cond, copy.start), lambda: when(got, copy.wait_recv)

    def shift(axis, sign, src, dst):
        return remote(src, dst, {axis: at[axis] + sign}, has[axis, sign], has[axis, -sign])

    def partner(src, dst, cond=None):
        return remote(src, dst, {"gz": other}, cond, cond)

    def zero(cond, ref):
        @pl.when(jnp.logical_not(cond))
        def _():
            ref[...] = jnp.zeros(ref.shape, ref.dtype)

    mid = slice(8, 8 + nx)
    zero(has["gx", -1], e.at[0])
    zero(has["gx", 1], e.at[nx + 1])
    zero(has["gy", -1], m.at[:, 0, mid])
    zero(top, m.at[:, ny_cells + 1, mid])
    zero(has["gx", -1], m.at[:, :, 0:8])
    zero(has["gx", 1], m.at[:, :, 8 + nx:16 + nx])
    g[nx + 2:] = jnp.zeros((g.shape[0] - nx - 2,) + g.shape[1:], bf16)
    zero(top, g.at[1:nx + 1])
    zero(jnp.logical_and(top, has["gx", -1]), g.at[0])
    zero(jnp.logical_and(top, has["gx", 1]), g.at[nx + 1])
    zero(top, cz_in)
    m[:, 1:ny_cells + 1, mid] = jnp.zeros((2, ny_cells, nx, LANES), f32)
    for f in range(2):
        for y in range(ny_cells):
            m[f, y + 1, mid, :size_z] = mat_ref[f, :, y, :]

    pl.semaphore_wait(barrier, total)

    my_down = shift("gy", -1, m.at[:, 1, mid], m.at[:, ny_cells + 1, mid])
    my_up = shift("gy", 1, m.at[:, ny_cells, mid], m.at[:, 0, mid])
    my_down[0]()
    my_up[0]()
    bounds = [(nx - 1, nx), (0, 1), (1, 3)] + [(a, min(a + 4, nx - 1)) for a in range(3, nx - 1, 4)]
    y_ghosts = [shift("gy", -1, v_ref.at[a:b, :size_z], g.at[a + 1:b + 1, :size_z]) for a, b in bounds]
    for copy in y_ghosts[:3]:
        copy[0]()
    x_down = shift("gx", -1, v_ref.at[0], e.at[nx + 1, GHOST:tail])
    x_up = shift("gx", 1, v_ref.at[nx - 1], e.at[0, GHOST:tail])

    edge = jnp.where(gz == 0, size_z - 1, 0)
    row = lax.broadcasted_iota(jnp.int32, (GHOST, own), 0)
    col = lax.broadcasted_iota(jnp.int32, (GHOST, own), 1)
    pick = jnp.logical_and(row < ny_cells, col == row * size_z + edge)
    pick = jnp.where(pick, 1.0, 0.0).astype(bf16)

    def take_edge(x):
        zs[x] = jnp.dot(pick, e[x, GHOST:tail], preferred_element_type=f32).astype(bf16)

    own_v.wait()

    def two_edges(i, carry):
        take_edge(2 * i + 1)
        take_edge(2 * i + 2)
        return carry

    lax.fori_loop(0, nx // 2, two_edges, 0)
    z_own = [partner(zs.at[1:nx + 1], e.at[1:nx + 1, :GHOST]),
             partner(zs.at[1:nx + 1], e.at[1:nx + 1, tail:])]
    for copy in z_own:
        copy[0]()
    row = lax.broadcasted_iota(jnp.int32, (nx, nx * GHOST), 0)
    col = lax.broadcasted_iota(jnp.int32, (nx, nx * GHOST), 1)
    pick2 = jnp.where(col == row * GHOST, 1.0, 0.0).astype(bf16)
    cz_out[...] = jnp.dot(pick2, zs[1:nx + 1].reshape(nx * GHOST, columns),
                          preferred_element_type=f32).astype(bf16)
    corner = remote(cz_out, cz_in, {"gy": gy - 1, "gz": other}, has["gy", -1], top)
    corner[0]()
    for copy in y_ghosts[3:]:
        copy[0]()
    my_down[1]()
    my_up[1]()
    mx_down = shift("gx", -1, m.at[:, :, 8:16], m.at[:, :, 8 + nx:16 + nx])
    mx_up = shift("gx", 1, m.at[:, :, nx:8 + nx], m.at[:, :, 0:8])
    mx_down[0]()
    mx_up[0]()
    x_down[0]()
    x_up[0]()

    own_t.wait()
    for copy in z_own:
        copy[1]()

    ring_size = pp.shape[0]

    def ring(x):
        return pp.at[x % ring_size]

    def taps_of(x, dst, *more):
        first = jnp.dot(t[0], e[x + 1, :kw], preferred_element_type=f32)
        second = jnp.dot(t[1], e[x + 1, tail + GHOST - kw:], preferred_element_type=f32)
        for ref in (dst,) + more:
            ref[:2 * hz] = first
            ref[2 * hz:] = second

    acc[...] = jnp.zeros_like(acc)
    taps_of(0, ring(0), ps0)
    taps_of(1, ring(1), ps1)
    for x in range(2, 4):
        taps_of(x, ring(x))
    mx_down[1]()
    mx_up[1]()
    mz_copy = partner(m, mz)
    mz_copy[0]()
    ready = ring_size - 1
    for x in range(4, ready):
        taps_of(x, ring(x))
    mz_copy[1]()

    lanes = lax.broadcasted_iota(jnp.int32, (m.shape[2], LANES), 1)
    turn = jnp.where(gz == 0, size_z - 1, LANES - size_z + 1)

    def z_sum(y):
        k = m[0, y]
        ghost = jnp.where(lanes == edge, pltpu.roll(mz[0, y], turn, 1), 0.0)
        return pltpu.roll(k, 1, 1) + 2.0 * k + pltpu.roll(k, LANES - 1, 1) + ghost

    sums = [z_sum(y) for y in range(ny_cells + 2)]
    for y in range(ny_cells):
        fy[y] = sums[y] + 2.0 * sums[y + 1] + sums[y + 2]
        field = fy[y, 7:7 + nx] + 2.0 * fy[y, 8:8 + nx] + fy[y, 9:9 + nx]
        kappa = m[0, y + 1, mid]
        rho = m[1, y + 1, mid]
        both = jnp.concatenate([2.0 * kappa + field * (1.0 / 32.0), kappa * (1.0 / 16.0),
                                rho * (1.0 / 216.0)], 0)
        cols[y, :, :3 * nx] = both.T[:size_z]

    wide = 2 * LANES
    dims = (((0,), (0,)), ((), ()))

    def column(x, y, c):
        one = jnp.broadcast_to(cols[y, :, c * nx + x:c * nx + x + 1], (size_z, LANES))
        return jnp.concatenate([one, one], 1)

    def values(x, before, now, after, dst, base):
        for y in range(ny_cells):
            h, yy = divmod(y, half)
            sr = slice(2 * hz * h + size_z * yy, 2 * hz * h + size_z * (yy + 1))
            mr = slice(sr.start + hz, sr.stop + hz)
            rr = slice(base + size_z * y, base + size_z * (y + 1))
            d, kq, rq = (column(x, y, c) for c in range(3))
            for at_lane in range(0, columns, wide):
                ll = slice(at_lane, at_lane + wide)
                v = e[x + 1, GHOST + size_z * y:GHOST + size_z * (y + 1), ll].astype(f32)
                s = before[sr, ll] + after[sr, ll] + 2.0 * now[sr, ll]
                w = before[mr, ll] + after[mr, ll] + 4.0 * now[mr, ll]
                dst[rr, ll] = (d * v - kq * s).astype(bf16)
                dst[rr, slice(columns + at_lane, columns + at_lane + wide)] = (rq * w).astype(bf16)

    def gram(first, second, src):
        v = jnp.concatenate([e[first + 1, GHOST:tail], e[second + 1, GHOST:tail]], 0)
        acc[...] += lax.dot_general(v, src[...], dims, preferred_element_type=f32)

    def relay(sign, src, dst):
        return remote(g.at[src, :size_z], g.at[dst, :size_z], {"gx": gx + sign},
                      jnp.logical_and(top, has["gx", sign]), jnp.logical_and(top, has["gx", -sign]))

    relays = [relay(-1, 1, nx + 1), relay(1, nx, 0)]
    z_ghosts = [partner(zs.at[x], e.at[x, at_row:at_row + GHOST])
                for x in (0, nx + 1) for at_row in (0, tail)]
    zrow = pl.multiple_of(jnp.where(gz == 0, size_z - GHOST, 0), GHOST)
    z_relays = [partner(g.at[j, pl.ds(zrow, GHOST)], g.at[j, size_z:], top) for j in (0, nx + 1)]

    def stage(n):
        if n == 3:
            for copy in y_ghosts[:2]:
                copy[1]()
            for copy in relays:
                copy[0]()
        elif n == 5:
            x_down[1]()
            x_up[1]()
            take_edge(0)
            take_edge(nx + 1)
            for copy in z_ghosts:
                copy[0]()
            for copy in relays:
                copy[1]()
            for copy in z_relays:
                copy[0]()
        elif n == 6:
            for copy in z_ghosts:
                copy[1]()

    pairs = [(x, x + 1) for x in range(1, nx - 1, 2)] + [(nx - 1, 0)]
    previous = None
    for n, pair in enumerate(pairs):
        stage(n)
        y_now = (ya, yb)[n % 2]
        for k, x in enumerate(pair):
            if x == nx - 1:
                refs = ring(x - 1), ring(x), ring(nx)
            elif x == 0:
                refs = ring(nx + 1), ps0, ps1
            else:
                refs = ring(x - 1), ring(x), ring(x + 1)
            values(x, *refs, y_now, k * own)
        for x in (ready + 2 * n, ready + 2 * n + 1):
            if x < nx:
                taps_of(x, ring(x))
        if n == 6:
            taps_of(nx, ring(nx))
            taps_of(-1, ring(nx + 1))
        if previous is not None:
            gram(*previous)
        previous = pair + (y_now,)
    gram(*previous)

    reach = jnp.where(gz == 0, size_z, GHOST)
    mine = lanes < size_z

    def ghost_columns(f, factor):
        k = m[f, ny_cells + 1]
        return jnp.where(mine, k, pltpu.roll(mz[f, ny_cells + 1], reach, 1)) * factor

    both = jnp.concatenate([ghost_columns(0, 1.0 / 16.0), ghost_columns(1, 1.0 / 216.0)], 0)
    ghost_cols = both.T[:group]
    for f in range(2):
        for j in range(nx + 2):
            n = f * m.shape[2] + 7 + j
            gc[f, j] = jnp.broadcast_to(ghost_cols[:, n:n + 1], (group, LANES))
    for copy in z_relays:
        copy[1]()
    corner[1]()
    for x in range(nx):
        one = cz_in[x:x + 1].astype(f32)
        g[x + 1, size_z:] = jnp.broadcast_to(one, (GHOST, columns)).astype(bf16)

    four_z = 4 * size_z

    def ghost_taps(n):
        at4 = slice(4 * n, 4 * n + 4)
        for k in range(4):
            j = 4 * n + k
            for at_lane in range(0, columns, LANES):
                ll = slice(at_lane, at_lane + LANES)
                if j < nx + 2:
                    v = g[j, :, ll].astype(f32)
                    gk[k, :, ll] = (v * gc[0, j]).astype(bf16)
                    gr[k, :, ll] = (v * gc[1, j]).astype(bf16)
                else:
                    gk[k, :, ll] = jnp.zeros((group, LANES), bf16)
                    gr[k, :, ll] = jnp.zeros((group, LANES), bf16)

        def put(kind, value):
            gg[kind, at4] = value.reshape(4, size_z, columns)

        first, second = t[2, :four_z, :4 * group], t[2, four_z:2 * four_z, :4 * group]
        raw = g[at4].reshape(4 * group, columns)
        put(0, jnp.dot(first, raw, preferred_element_type=f32))
        put(1, jnp.dot(second, raw, preferred_element_type=f32))
        put(2, jnp.dot(first, gk[...].reshape(4 * group, columns), preferred_element_type=f32))
        put(3, jnp.dot(second, gr[...].reshape(4 * group, columns), preferred_element_type=f32))

    def late(x):
        def three(kind, middle, ll):
            return gg[kind, x, :, ll] + gg[kind, x + 2, :, ll] + middle * gg[kind, x + 1, :, ll]

        kq, rq = column(x, ny_cells - 1, 1), column(x, ny_cells - 1, 2)
        for at_lane in range(0, columns, wide):
            ll = slice(at_lane, at_lane + wide)
            s = kq * three(0, 2.0, ll) + three(2, 2.0, ll)
            w = rq * three(1, 4.0, ll) + three(3, 4.0, ll)
            yl[x, :, ll] = (-s).astype(bf16)
            yl[x, :, slice(columns + at_lane, columns + at_lane + wide)] = w.astype(bf16)

    def late_gram(first, stop):
        v = jnp.concatenate([e[x + 1, tail - size_z:tail] for x in range(first, stop)], 0)
        y = yl[first:stop].reshape((stop - first) * size_z, 2 * columns)
        acc[...] += lax.dot_general(v, y, dims, preferred_element_type=f32)

    ghost_taps(nx // 4)
    done_to, made_to = 0, 0
    for n in range(nx // 4):
        y_ghosts[2 + n][1]()
        ghost_taps(n)
        make_to = nx if n == nx // 4 - 1 else 4 * n + 2
        for x in range(made_to, make_to):
            late(x)
        made_to = make_to
        if made_to == nx or made_to - done_to > 4:
            stop = made_to if made_to == nx else done_to + 5
            late_gram(done_to, stop)
            done_to = stop

    rows = out_ref.shape[0]

    def symmetric(side):
        ll = slice(side * columns, (side + 1) * columns)
        a = acc[:, ll]
        a = (a + a.T) * scale
        for n in range(columns // rows):
            i, rest = divmod(n, cy * cz)
            j, k = divmod(rest, cz)
            part[i, j, k, :, ll] = a[n * rows:(n + 1) * rows]

    def everywhere(axis, piece, landing):
        count = lax.axis_size(axis)
        me = lax.axis_index(axis)
        copies = []
        for k in range(1, count):
            peer = lax.rem(me + k, count)
            copy = remote(piece(peer), landing.at[k - 1], {axis: peer})
            copy[0]()
            copies.append(copy)
        return copies

    def collect(copies, held, landing):
        for copy in copies:
            copy[1]()
        for k in range(len(copies)):
            held = held + landing[k]
        return held

    flights = []
    for n, (lo, hi, by) in enumerate(chunks):
        for side in range(2):
            if lo <= side * columns < hi:
                symmetric(side)
        rz = buffers[n][0]
        flights.append(everywhere("gz", lambda p, lo=lo, hi=hi: part.at[:, :, p, :, lo:hi], rz))
    for n, (lo, hi, by) in enumerate(chunks):
        rz, s1, r1, s2, r2 = buffers[n]
        s1[...] = collect(flights[n], part[:, :, gz, :, lo:hi], rz)
        if by == "gy":
            flights[n] = everywhere("gy", lambda p, s1=s1: s1.at[:, p], r1)
        else:
            flights[n] = everywhere("gx", lambda p, s1=s1: s1.at[p], r1)
    for n, (lo, hi, by) in enumerate(chunks):
        rz, s1, r1, s2, r2 = buffers[n]
        mine_now = s1[:, gy] if by == "gy" else s1[gx]
        s2[...] = collect(flights[n], mine_now, r1)
        flights[n] = everywhere("gx" if by == "gy" else "gy", lambda p, s2=s2: s2.at[p], r2)
    for n, (lo, hi, by) in enumerate(chunks):
        rz, s1, r1, s2, r2 = buffers[n]
        out_ref[:, lo:hi] = collect(flights[n], s2[gx] if by == "gy" else s2[gy], r2)
    for done in sent:
        done()


def per_device(eigvecs, material):
    size_x, size_y, size_z, columns = eigvecs.shape
    nx, ny, nz = (lax.axis_size(a) for a in ("gx", "gy", "gz"))
    total_cells = size_x * size_y * size_z * nx * ny * nz
    own = size_y * size_z
    tail = own + 2 * GHOST
    group = size_z + GHOST
    rows = columns // (nx * ny * nz)
    wide = 2 * columns
    matrices = jnp.asarray(tap_matrices(size_y, size_z), jnp.bfloat16)
    parts = ((3, "gy"), (2, "gx"), (2, "gy"), (1, "gx"))
    unit = wide // 8
    chunks, lo = [], 0
    for width, by in parts:
        chunks.append((lo, lo + width * unit, by))
        lo += width * unit
    f32, bf16 = jnp.float32, jnp.bfloat16
    dma = pltpu.SemaphoreType.DMA
    vmem = pl.BlockSpec(memory_space=pltpu.VMEM)
    anywhere = pl.BlockSpec(memory_space=pl.ANY)
    late_planes = -(-(size_x + 2) // 4) * 4
    copies = 48 + len(chunks) * (nx + ny + nz - 3)
    plane = ((2 * own, columns), f32)
    scratch = [
        ((size_x + 2, tail, columns), bf16),
        ((10, 2 * own, columns), f32), plane, plane,
        ((2 * own, wide), bf16), ((2 * own, wide), bf16),
        ((columns, wide), f32),
        (matrices.shape[1:], bf16),
        ((size_x + 2, GHOST, columns), bf16),
        ((size_x, columns), bf16),
        ((size_x, columns), bf16),
        ((2, size_y + 2, size_x + 16, LANES), f32),
        ((2, size_y + 2, size_x + 16, LANES), f32),
        ((size_y, size_x + 16, LANES), f32),
        ((size_y, size_z, LANES), f32),
        ((2, size_x + 2, group, LANES), f32),
        ((late_planes, group, columns), bf16),
        ((4, group, columns), bf16),
        ((4, group, columns), bf16),
        ((4, late_planes, size_z, columns), f32),
        ((size_x, size_z, wide), bf16),
        ((nx, ny, nz, rows, wide), f32),
    ]
    for low, high, by in chunks:
        w = high - low
        n1, n2 = (ny, nx) if by == "gy" else (nx, ny)
        scratch += [((nz - 1, nx, ny, rows, w), f32), ((nx, ny, rows, w), f32),
                    ((n1 - 1, n2, rows, w), f32), ((n2, rows, w), f32), ((n2 - 1, rows, w), f32)]
    out = pl.pallas_call(
        functools.partial(kernel, 0.5 / total_cells, tuple(chunks)),
        out_shape=jax.ShapeDtypeStruct((rows, wide), f32),
        in_specs=[anywhere, vmem, anywhere],
        out_specs=vmem,
        scratch_shapes=[pltpu.VMEM(*s) for s in scratch] + [dma((2,)), dma((copies,)), dma((copies,))],
        compiler_params=pltpu.CompilerParams(
            vmem_limit_bytes=63 * 1024 * 1024, collective_id=0, has_side_effects=True),
    )(eigvecs.reshape(size_x, own, columns), material, matrices)
    return out[:, :columns], out[:, columns:]


def solution(mesh):
    return jax.shard_map(
        per_device,
        mesh=mesh,
        in_specs=(P("gx", "gy", "gz", None), P(None, "gx", "gy", "gz")),
        out_specs=(P(("gx", "gy", "gz"), None), P(("gx", "gy", "gz"), None)),
        check_vma=False,
    )
```

```python
import functools
import numpy as np
import jax
import jax.numpy as jnp
from jax import lax
from jax.experimental import pallas as pl
from jax.experimental.pallas import tpu as pltpu
from jax.sharding import PartitionSpec as P

LANES = 128
GHOST = 16
MESH = pl.DeviceIdType.MESH
AXES = ("gx", "gy", "gz")


def tap(a, b, middle):
    return middle if a == b else (1.0 if abs(a - b) == 1 else 0.0)


def tap_matrices(size_y, size_z):
    half = size_y // 2
    width = (half + 1) * size_z + GHOST
    sides = []
    for side in (0, 1):
        edge = size_z - 1 if side == 0 else 0
        blocks = []
        for first in (0, 1):
            ys_in = range(0, half + 1) if first == 0 else range(half - 1, size_y)
            ys_out = range(0, half) if first == 0 else range(half, size_y)
            own_at = GHOST if first == 0 else 0
            ghost_at = 0 if first == 0 else (half + 1) * size_z
            rows = []
            for middle in (2.0, 4.0):
                zz = middle * np.eye(size_z) + np.eye(size_z, k=1) + np.eye(size_z, k=-1)
                block = np.zeros((half * size_z, width))
                for o, y in enumerate(ys_out):
                    for n, y2 in enumerate(ys_in):
                        w = tap(y, y2, middle)
                        if w:
                            block[o * size_z:(o + 1) * size_z,
                                  own_at + n * size_z:own_at + (n + 1) * size_z] = w * zz
                            block[o * size_z + edge, ghost_at + y2] = w
                rows.append(block)
            blocks.append(np.concatenate(rows, 0))
        group = size_z + GHOST
        rows = []
        for middle in (2.0, 4.0):
            zz = middle * np.eye(size_z) + np.eye(size_z, k=1) + np.eye(size_z, k=-1)
            one = np.zeros((size_z, group))
            one[:, :size_z] = zz
            one[edge, size_z + (0 if side == 0 else GHOST - 1)] = 1.0
            rows.append(np.kron(np.eye(4), one))
        late = np.concatenate(rows, 0)
        full = np.zeros((blocks[0].shape[0], width))
        full[:late.shape[0], :late.shape[1]] = late
        blocks.append(full)
        sides.append(np.stack(blocks))
    return np.stack(sides)


def kernel(scale, chunks, v_ref, mat_ref, t_hbm, out_ref,
           mat, xf_out, xf_in, e, pp, ps0, ps1, ya, yb, acc, t, zs, cz_out, cz_in, m, mz, fy, cols, gc, g, gk, gr, gg, yl,
           part, *rest):
    f32, bf16 = jnp.float32, jnp.bfloat16
    local, send, recv = rest[-3:]
    buffers = [rest[5 * n:5 * n + 5] for n in range(len(chunks))]
    nx, own, columns = v_ref.shape
    ny_cells, size_z = mat.shape[2:]
    half = ny_cells // 2
    group = size_z + GHOST
    hz = half * size_z
    kw = t.shape[2]
    tail = GHOST + own
    gx, gy, gz = (lax.axis_index(a) for a in AXES)
    cx, cy, cz = (lax.axis_size(a) for a in AXES)
    has = {("gx", -1): gx > 0, ("gx", 1): gx < cx - 1, ("gy", -1): gy > 0, ("gy", 1): gy < cy - 1}
    at = {"gx": gx, "gy": gy}
    top = has["gy", 1]
    other = lax.rem(gz + 1, cz)
    barrier = pltpu.get_barrier_semaphore()
    total = 0
    for axis, count in (("gz", cz), ("gy", cy), ("gx", cx)):
        me = lax.axis_index(axis)
        for k in range(1, count):
            pl.semaphore_signal(barrier, inc=1, device_id={axis: lax.rem(me + k, count)},
                                device_id_type=MESH)
        total += count - 1
    for sign in (-1, 1):
        @pl.when(has["gy", sign])
        def _(sign=sign):
            pl.semaphore_signal(barrier, inc=1, device_id={"gy": gy + sign, "gz": other},
                                device_id_type=MESH)
        total = total + jnp.where(has["gy", sign], 1, 0)

    own_m = pltpu.make_async_copy(mat_ref, mat, local.at[0])
    own_m.start()
    step = nx // 4
    own_v = [pltpu.make_async_copy(v_ref.at[n * step:(n + 1) * step],
                                   e.at[1 + n * step:1 + (n + 1) * step, GHOST:tail], local.at[2 + n])
             for n in range(4)]
    for copy in own_v:
        copy.start()
    own_t = pltpu.make_async_copy(t_hbm.at[gz], t, local.at[1])
    own_t.start()

    used = [0]
    sent = []

    def remote(src, dst, device, cond=None, got=None):
        n = used[0]
        used[0] += 1
        copy = pltpu.make_async_remote_copy(src_ref=src, dst_ref=dst, send_sem=send.at[n],
                                            recv_sem=recv.at[n], device_id=device,
                                            device_id_type=MESH)

        def when(test, action):
            if test is None:
                action()
            else:
                pl.when(test)(action)

        sent.append(lambda: when(cond, copy.wait_send))
        return lambda: when(cond, copy.start), lambda: when(got, copy.wait_recv)

    def shift(axis, sign, src, dst):
        return remote(src, dst, {axis: at[axis] + sign}, has[axis, sign], has[axis, -sign])

    def partner(src, dst, cond=None):
        return remote(src, dst, {"gz": other}, cond, cond)

    def zero(cond, ref):
        @pl.when(jnp.logical_not(cond))
        def _():
            ref[...] = jnp.zeros(ref.shape, ref.dtype)

    mid = slice(8, 8 + nx)
    zero(has["gx", -1], e.at[0])
    zero(has["gx", 1], e.at[nx + 1])
    zero(has["gy", -1], m.at[:, 0, mid])
    zero(top, m.at[:, ny_cells + 1, mid])
    zero(has["gx", -1], xf_in.at[1])
    zero(has["gx", 1], xf_in.at[0])
    for at_row in (0, 8 + nx):
        m[:, :, at_row:at_row + 8] = jnp.zeros((2, ny_cells + 2, 8, LANES), f32)
    xf_out[...] = jnp.zeros(xf_out.shape, f32)
    g[nx + 2:] = jnp.zeros((g.shape[0] - nx - 2,) + g.shape[1:], bf16)
    zero(top, g.at[1:nx + 1])
    zero(jnp.logical_and(top, has["gx", -1]), g.at[0])
    zero(jnp.logical_and(top, has["gx", 1]), g.at[nx + 1])
    zero(top, cz_in)
    m[:, 1:ny_cells + 1, mid] = jnp.zeros((2, ny_cells, nx, LANES), f32)
    own_m.wait()
    for f in range(2):
        for y in range(ny_cells):
            m[f, y + 1, mid, :size_z] = mat[f, :, y, :]

    pl.semaphore_wait(barrier, total)

    my_down = shift("gy", -1, m.at[:, 1, mid], m.at[:, ny_cells + 1, mid])
    my_up = shift("gy", 1, m.at[:, ny_cells, mid], m.at[:, 0, mid])
    my_down[0]()
    my_up[0]()
    bounds = [(nx - 1, nx), (0, 1), (1, 3)] + [(a, min(a + 4, nx - 1)) for a in range(3, nx - 1, 4)]
    y_ghosts = [shift("gy", -1, v_ref.at[a:b, :size_z], g.at[a + 1:b + 1, :size_z]) for a, b in bounds]
    for copy in y_ghosts[:3]:
        copy[0]()
    x_down = shift("gx", -1, v_ref.at[0], e.at[nx + 1, GHOST:tail])
    x_up = shift("gx", 1, v_ref.at[nx - 1], e.at[0, GHOST:tail])

    edge = jnp.where(gz == 0, size_z - 1, 0)
    row = lax.broadcasted_iota(jnp.int32, (GHOST, own), 0)
    col = lax.broadcasted_iota(jnp.int32, (GHOST, own), 1)
    pick = jnp.logical_and(row < ny_cells, col == row * size_z + edge)
    pick = jnp.where(pick, 1.0, 0.0).astype(bf16)

    def take_edge(x):
        zs[x] = jnp.dot(pick, e[x, GHOST:tail], preferred_element_type=f32).astype(bf16)

    z_own = []
    for n in range(4):
        own_v[n].wait()
        low, high = 1 + n * step, 1 + (n + 1) * step
        for x in range(low, high):
            take_edge(x)
        z_own.append([partner(zs.at[low:high], e.at[low:high, :GHOST]),
                      partner(zs.at[low:high], e.at[low:high, tail:])])
        for copy in z_own[n]:
            copy[0]()
    my_down[1]()
    my_up[1]()
    count_y = ny_cells + 2
    for f in range(2):
        xf_out[0, f, :count_y] = m[f, :, 8, :]
        xf_out[1, f, :count_y] = m[f, :, 7 + nx, :]
    mx_down = shift("gx", -1, xf_out.at[0], xf_in.at[0])
    mx_up = shift("gx", 1, xf_out.at[1], xf_in.at[1])
    mx_down[0]()
    mx_up[0]()
    x_down[0]()
    x_up[0]()
    row = lax.broadcasted_iota(jnp.int32, (nx, nx * GHOST), 0)
    col = lax.broadcasted_iota(jnp.int32, (nx, nx * GHOST), 1)
    pick2 = jnp.where(col == row * GHOST, 1.0, 0.0).astype(bf16)
    cz_out[...] = jnp.dot(pick2, zs[1:nx + 1].reshape(nx * GHOST, columns),
                          preferred_element_type=f32).astype(bf16)
    corner = remote(cz_out, cz_in, {"gy": gy - 1, "gz": other}, has["gy", -1], top)
    corner[0]()
    for copy in y_ghosts[3:]:
        copy[0]()
    own_t.wait()

    ring_size = pp.shape[0]

    def ring(x):
        return pp.at[x % ring_size]

    def taps_of(x, dst, *more):
        first = jnp.dot(t[0], e[x + 1, :kw], preferred_element_type=f32)
        second = jnp.dot(t[1], e[x + 1, tail + GHOST - kw:], preferred_element_type=f32)
        for ref in (dst,) + more:
            ref[:2 * hz] = first
            ref[2 * hz:] = second

    acc[...] = jnp.zeros_like(acc)
    def arrived(n):
        for copy in z_own[n]:
            copy[1]()

    arrived(0)
    taps_of(0, ring(0), ps0)
    taps_of(1, ring(1), ps1)
    for x in range(2, step):
        taps_of(x, ring(x))
    mx_down[1]()
    mx_up[1]()
    for f in range(2):
        for y in range(count_y):
            m[f, y, 8 + nx:9 + nx] = xf_in[0, f, y:y + 1]
            m[f, y, 7:8] = xf_in[1, f, y:y + 1]
    arrived(1)
    for x in range(step, step + 2):
        taps_of(x, ring(x))
    mz_copy = partner(m, mz)
    mz_copy[0]()
    for n in range(2, 4):
        arrived(n)
    ready = ring_size - 1
    for x in range(step + 2, ready):
        taps_of(x, ring(x))
    mz_copy[1]()

    lanes = lax.broadcasted_iota(jnp.int32, (m.shape[2], LANES), 1)
    turn = jnp.where(gz == 0, size_z - 1, LANES - size_z + 1)

    def z_sum(y):
        k = m[0, y]
        ghost = jnp.where(lanes == edge, pltpu.roll(mz[0, y], turn, 1), 0.0)
        return pltpu.roll(k, 1, 1) + 2.0 * k + pltpu.roll(k, LANES - 1, 1) + ghost

    sums = [z_sum(y) for y in range(ny_cells + 2)]
    for y in range(ny_cells):
        fy[y] = sums[y] + 2.0 * sums[y + 1] + sums[y + 2]
        field = fy[y, 7:7 + nx] + 2.0 * fy[y, 8:8 + nx] + fy[y, 9:9 + nx]
        kappa = m[0, y + 1, mid]
        rho = m[1, y + 1, mid]
        both = jnp.concatenate([2.0 * kappa + field * (1.0 / 32.0), kappa * (1.0 / 16.0),
                                rho * (1.0 / 216.0)], 0)
        cols[y, :, :3 * nx] = both.T[:size_z]

    dims = (((0,), (0,)), ((), ()))

    def column(x, y, c):
        return jnp.broadcast_to(cols[y, :, c * nx + x:c * nx + x + 1], (size_z, LANES))

    def values(xs, planes, dst, base=0):
        for y in range(ny_cells):
            h, yy = divmod(y, half)
            sr = slice(2 * hz * h + size_z * yy, 2 * hz * h + size_z * (yy + 1))
            mr = slice(sr.start + hz, sr.stop + hz)
            coef = [[column(x, y, c) for c in range(3)] for x in xs]
            for at_lane in range(0, columns, LANES):
                ll = slice(at_lane, at_lane + LANES)
                p = [ref[sr, ll] for ref in planes]
                q = [ref[mr, ll] for ref in planes]
                for k, x in enumerate(xs):
                    d, kq, rq = coef[k]
                    rr = slice(base + k * own + size_z * y, base + k * own + size_z * (y + 1))
                    v = e[x + 1, GHOST + size_z * y:GHOST + size_z * (y + 1), ll].astype(f32)
                    s = p[k] + p[k + 2] + 2.0 * p[k + 1]
                    w = q[k] + q[k + 2] + 4.0 * q[k + 1]
                    dst[rr, ll] = (d * v - kq * s).astype(bf16)
                    dst[rr, slice(columns + at_lane, columns + at_lane + LANES)] = (rq * w).astype(bf16)

    def gram(first, second, src):
        v = jnp.concatenate([e[first + 1, GHOST:tail], e[second + 1, GHOST:tail]], 0)
        acc[...] += lax.dot_general(v, src[...], dims, preferred_element_type=f32)

    def relay(sign, src, dst):
        return remote(g.at[src, :size_z], g.at[dst, :size_z], {"gx": gx + sign},
                      jnp.logical_and(top, has["gx", sign]), jnp.logical_and(top, has["gx", -sign]))

    relays = [relay(-1, 1, nx + 1), relay(1, nx, 0)]
    z_ghosts = [partner(zs.at[x], e.at[x, at_row:at_row + GHOST])
                for x in (0, nx + 1) for at_row in (0, tail)]
    zrow = pl.multiple_of(jnp.where(gz == 0, size_z - GHOST, 0), GHOST)
    z_relays = [partner(g.at[j, pl.ds(zrow, GHOST)], g.at[j, size_z:], top) for j in (0, nx + 1)]

    reach = jnp.where(gz == 0, size_z, GHOST)
    mine = lanes < size_z

    def ghost_columns(f, factor):
        k = m[f, ny_cells + 1]
        return jnp.where(mine, k, pltpu.roll(mz[f, ny_cells + 1], reach, 1)) * factor

    def prepare_ghosts():
        both = jnp.concatenate([ghost_columns(0, 1.0 / 16.0), ghost_columns(1, 1.0 / 216.0)], 0)
        ghost_cols = both.T[:group]
        for f in range(2):
            for j in range(nx + 2):
                n = f * m.shape[2] + 7 + j
                gc[f, j] = jnp.broadcast_to(ghost_cols[:, n:n + 1], (group, LANES))
        for x in range(nx):
            one = cz_in[x:x + 1].astype(f32)
            g[x + 1, size_z:] = jnp.broadcast_to(one, (GHOST, columns)).astype(bf16)

    four_z = 4 * size_z

    def ghost_taps(n):
        at4 = slice(4 * n, 4 * n + 4)
        for k in range(4):
            j = 4 * n + k
            for at_lane in range(0, columns, LANES):
                ll = slice(at_lane, at_lane + LANES)
                if j < nx + 2:
                    v = g[j, :, ll].astype(f32)
                    gk[k, :, ll] = (v * gc[0, j]).astype(bf16)
                    gr[k, :, ll] = (v * gc[1, j]).astype(bf16)
                else:
                    gk[k, :, ll] = jnp.zeros((group, LANES), bf16)
                    gr[k, :, ll] = jnp.zeros((group, LANES), bf16)

        def put(kind, value):
            gg[kind, at4] = value.reshape(4, size_z, columns)

        first, second = t[2, :four_z, :4 * group], t[2, four_z:2 * four_z, :4 * group]
        raw = g[at4].reshape(4 * group, columns)
        put(0, jnp.dot(first, raw, preferred_element_type=f32))
        put(1, jnp.dot(second, raw, preferred_element_type=f32))
        put(2, jnp.dot(first, gk[...].reshape(4 * group, columns), preferred_element_type=f32))
        put(3, jnp.dot(second, gr[...].reshape(4 * group, columns), preferred_element_type=f32))

    def late(x):
        def three(kind, middle, ll):
            return gg[kind, x, :, ll] + gg[kind, x + 2, :, ll] + middle * gg[kind, x + 1, :, ll]

        kq, rq = column(x, ny_cells - 1, 1), column(x, ny_cells - 1, 2)
        for at_lane in range(0, columns, LANES):
            ll = slice(at_lane, at_lane + LANES)
            s = kq * three(0, 2.0, ll) + three(2, 2.0, ll)
            w = rq * three(1, 4.0, ll) + three(3, 4.0, ll)
            yl[x, :, ll] = (-s).astype(bf16)
            yl[x, :, slice(columns + at_lane, columns + at_lane + LANES)] = w.astype(bf16)

    def late_gram(first, stop):
        v = jnp.concatenate([e[x + 1, tail - size_z:tail] for x in range(first, stop)], 0)
        y = yl[first:stop].reshape((stop - first) * size_z, 2 * columns)
        acc[...] += lax.dot_general(v, y, dims, preferred_element_type=f32)

    def stage(n):
        if n == 3:
            for copy in y_ghosts[:2]:
                copy[1]()
            for copy in relays:
                copy[0]()
        elif n == 5:
            x_down[1]()
            x_up[1]()
            take_edge(0)
            take_edge(nx + 1)
            for copy in z_ghosts:
                copy[0]()
            for copy in relays:
                copy[1]()
            for copy in z_relays:
                copy[0]()
        elif n == 6:
            for copy in z_ghosts:
                copy[1]()
            corner[1]()
        elif n == 7:
            for copy in z_relays:
                copy[1]()
            for copy in y_ghosts[2:5]:
                copy[1]()

    pairs = [(x, x + 1) for x in range(1, nx - 1, 2)] + [(nx - 1, 0)]
    previous = None
    for n, pair in enumerate(pairs):
        stage(n)
        y_now = (ya, yb)[n % 2]
        if pair[1]:
            values(pair, [ring(x) for x in range(pair[0] - 1, pair[1] + 2)], y_now)
        else:
            values((nx - 1,), [ring(nx - 2), ring(nx - 1), ring(nx)], y_now)
            values((0,), [ring(nx + 1), ps0, ps1], y_now, own)
        for x in (ready + 2 * n, ready + 2 * n + 1):
            if x < nx:
                taps_of(x, ring(x))
        if n == 6:
            taps_of(nx, ring(nx))
            taps_of(-1, ring(nx + 1))
        if n == 6:
            prepare_ghosts()
        if previous is not None:
            gram(*previous)
        previous = pair + (y_now,)
    for n in (nx // 4, 0):
        ghost_taps(n)
    gram(*previous)

    done_to, made_to = 0, 0
    for n in range(nx // 4):
        if n == 3:
            y_ghosts[5][1]()
        if n:
            ghost_taps(n)
        make_to = nx if n == nx // 4 - 1 else 4 * n + 2
        for x in range(made_to, make_to):
            late(x)
        made_to = make_to
        if made_to == nx or made_to - done_to > 4:
            stop = made_to if made_to == nx else done_to + 5
            late_gram(done_to, stop)
            done_to = stop

    rows = out_ref.shape[0]

    def symmetric(side):
        ll = slice(side * columns, (side + 1) * columns)
        a = acc[:, ll]
        a = (a + a.T) * scale
        for n in range(columns // rows):
            i, rest = divmod(n, cy * cz)
            j, k = divmod(rest, cz)
            part[i, j, k, :, ll] = a[n * rows:(n + 1) * rows]

    def everywhere(axis, piece, landing):
        count = lax.axis_size(axis)
        me = lax.axis_index(axis)
        copies = []
        for k in range(1, count):
            peer = lax.rem(me + k, count)
            copy = remote(piece(peer), landing.at[k - 1], {axis: peer})
            copy[0]()
            copies.append(copy)
        return copies

    def collect(copies, held, landing):
        for copy in copies:
            copy[1]()
        for k in range(len(copies)):
            held = held + landing[k]
        return held

    flights = []
    for n, (lo, hi, by) in enumerate(chunks):
        for side in range(2):
            if lo <= side * columns < hi:
                symmetric(side)
        rz = buffers[n][0]
        flights.append(everywhere("gz", lambda p, lo=lo, hi=hi: part.at[:, :, p, :, lo:hi], rz))
    for n, (lo, hi, by) in enumerate(chunks):
        rz, s1, r1, s2, r2 = buffers[n]
        s1[...] = collect(flights[n], part[:, :, gz, :, lo:hi], rz)
        if by == "gy":
            flights[n] = everywhere("gy", lambda p, s1=s1: s1.at[:, p], r1)
        else:
            flights[n] = everywhere("gx", lambda p, s1=s1: s1.at[p], r1)
    for n, (lo, hi, by) in enumerate(chunks):
        rz, s1, r1, s2, r2 = buffers[n]
        mine_now = s1[:, gy] if by == "gy" else s1[gx]
        s2[...] = collect(flights[n], mine_now, r1)
        flights[n] = everywhere("gx" if by == "gy" else "gy", lambda p, s2=s2: s2.at[p], r2)
    for n, (lo, hi, by) in enumerate(chunks):
        rz, s1, r1, s2, r2 = buffers[n]
        out_ref[:, lo:hi] = collect(flights[n], s2[gx] if by == "gy" else s2[gy], r2)
    for done in sent:
        done()


def per_device(eigvecs, material):
    size_x, size_y, size_z, columns = eigvecs.shape
    nx, ny, nz = (lax.axis_size(a) for a in ("gx", "gy", "gz"))
    total_cells = size_x * size_y * size_z * nx * ny * nz
    own = size_y * size_z
    tail = own + 2 * GHOST
    group = size_z + GHOST
    rows = columns // (nx * ny * nz)
    wide = 2 * columns
    matrices = jnp.asarray(tap_matrices(size_y, size_z), jnp.bfloat16)
    parts = ((2, "gy"), (2, "gx"), (2, "gy"), (1, "gy"), (1, "gy"))
    unit = wide // 8
    chunks, lo = [], 0
    for width, by in parts:
        chunks.append((lo, lo + width * unit, by))
        lo += width * unit
    f32, bf16 = jnp.float32, jnp.bfloat16
    dma = pltpu.SemaphoreType.DMA
    vmem = pl.BlockSpec(memory_space=pltpu.VMEM)
    anywhere = pl.BlockSpec(memory_space=pl.ANY)
    late_planes = -(-(size_x + 2) // 4) * 4
    copies = 48 + len(chunks) * (nx + ny + nz - 3)
    plane = ((2 * own, columns), f32)
    face = ((2, 2, GHOST, LANES), f32)
    scratch = [
        (material.shape, f32), face, face,
        ((size_x + 2, tail, columns), bf16),
        ((12, 2 * own, columns), f32), plane, plane,
        ((2 * own, wide), bf16), ((2 * own, wide), bf16),
        ((columns, wide), f32),
        (matrices.shape[1:], bf16),
        ((size_x + 2, GHOST, columns), bf16),
        ((size_x, columns), bf16),
        ((size_x, columns), bf16),
        ((2, size_y + 2, size_x + 16, LANES), f32),
        ((2, size_y + 2, size_x + 16, LANES), f32),
        ((size_y, size_x + 16, LANES), f32),
        ((size_y, size_z, LANES), f32),
        ((2, size_x + 2, group, LANES), f32),
        ((late_planes, group, columns), bf16),
        ((4, group, columns), bf16),
        ((4, group, columns), bf16),
        ((4, late_planes, size_z, columns), f32),
        ((size_x, size_z, wide), bf16),
        ((nx, ny, nz, rows, wide), f32),
    ]
    for low, high, by in chunks:
        w = high - low
        n1, n2 = (ny, nx) if by == "gy" else (nx, ny)
        scratch += [((nz - 1, nx, ny, rows, w), f32), ((nx, ny, rows, w), f32),
                    ((n1 - 1, n2, rows, w), f32), ((n2, rows, w), f32), ((n2 - 1, rows, w), f32)]
    out = pl.pallas_call(
        functools.partial(kernel, 0.5 / total_cells, tuple(chunks)),
        out_shape=jax.ShapeDtypeStruct((rows, wide), f32),
        in_specs=[anywhere] * 3,
        out_specs=vmem,
        scratch_shapes=[pltpu.VMEM(*s) for s in scratch] + [dma((6,)), dma((copies,)), dma((copies,))],
        compiler_params=pltpu.CompilerParams(
            vmem_limit_bytes=63 * 1024 * 1024, collective_id=0, has_side_effects=True),
    )(eigvecs.reshape(size_x, own, columns), material, matrices)
    return out[:, :columns], out[:, columns:]


def solution(mesh):
    return jax.shard_map(
        per_device,
        mesh=mesh,
        in_specs=(P("gx", "gy", "gz", None), P(None, "gx", "gy", "gz")),
        out_specs=(P(("gx", "gy", "gz"), None), P(("gx", "gy", "gz"), None)),
        check_vma=False,
    )
```

```python
import functools
import numpy as np
import jax
import jax.numpy as jnp
from jax import lax
from jax.experimental import pallas as pl
from jax.experimental.pallas import tpu as pltpu
from jax.sharding import PartitionSpec as P

LANES = 128
GHOST = 16
MESH = pl.DeviceIdType.MESH
AXES = ("gx", "gy", "gz")


def tap(a, b, middle):
    return middle if a == b else (1.0 if abs(a - b) == 1 else 0.0)


def tap_matrices(size_y, size_z):
    half = size_y // 2
    width = (half + 1) * size_z + GHOST
    sides = []
    for side in (0, 1):
        edge = size_z - 1 if side == 0 else 0
        blocks = []
        for first in (0, 1):
            ys_in = range(0, half + 1) if first == 0 else range(half - 1, size_y)
            ys_out = range(0, half) if first == 0 else range(half, size_y)
            own_at = GHOST if first == 0 else 0
            ghost_at = 0 if first == 0 else (half + 1) * size_z
            rows = []
            for middle in (2.0, 4.0):
                zz = middle * np.eye(size_z) + np.eye(size_z, k=1) + np.eye(size_z, k=-1)
                block = np.zeros((half * size_z, width))
                for o, y in enumerate(ys_out):
                    for n, y2 in enumerate(ys_in):
                        w = tap(y, y2, middle)
                        if w:
                            block[o * size_z:(o + 1) * size_z,
                                  own_at + n * size_z:own_at + (n + 1) * size_z] = w * zz
                            block[o * size_z + edge, ghost_at + y2] = w
                rows.append(block)
            blocks.append(np.concatenate(rows, 0))
        group = size_z + GHOST
        rows = []
        for middle in (2.0, 4.0):
            one = np.zeros((size_z, group))
            one[:, :size_z] = middle * np.eye(size_z) + np.eye(size_z, k=1) + np.eye(size_z, k=-1)
            one[edge, size_z + (0 if side == 0 else GHOST - 1)] = 1.0
            along = np.array([[tap(o + 1, j, middle) for j in range(4)] for o in range(2)])
            rows.append(np.kron(along, one))
        late = np.concatenate(rows, 0)
        full = np.zeros((blocks[0].shape[0], width))
        full[:late.shape[0], :late.shape[1]] = late
        blocks.append(full)
        sides.append(np.stack(blocks))
    return np.stack(sides)


def kernel(scale, chunks, v_ref, mat_ref, t_hbm, out_ref,
           mat, xf_out, xf_in, c_out, c_in, e, pp, ps0, ps1, ya, yb, acc, t, zs, cz_out, cz_in, m, mz, fy, cols, gc, g, gk, gr, yl,
           part, *rest):
    f32, bf16 = jnp.float32, jnp.bfloat16
    local, send, recv = rest[-3:]
    buffers = [rest[5 * n:5 * n + 5] for n in range(len(chunks))]
    nx, own, columns = v_ref.shape
    ny_cells, size_z = mat.shape[2:]
    half = ny_cells // 2
    group = size_z + GHOST
    hz = half * size_z
    kw = t.shape[2]
    tail = GHOST + own
    gx, gy, gz = (lax.axis_index(a) for a in AXES)
    cx, cy, cz = (lax.axis_size(a) for a in AXES)
    has = {("gx", -1): gx > 0, ("gx", 1): gx < cx - 1, ("gy", -1): gy > 0, ("gy", 1): gy < cy - 1}
    at = {"gx": gx, "gy": gy}
    top = has["gy", 1]
    other = lax.rem(gz + 1, cz)
    barrier = pltpu.get_barrier_semaphore()
    total = 0
    for axis, count in (("gz", cz), ("gy", cy), ("gx", cx)):
        me = lax.axis_index(axis)
        for k in range(1, count):
            pl.semaphore_signal(barrier, inc=1, device_id={axis: lax.rem(me + k, count)},
                                device_id_type=MESH)
        total += count - 1
    for sign in (-1, 1):
        @pl.when(has["gy", sign])
        def _(sign=sign):
            pl.semaphore_signal(barrier, inc=1, device_id={"gy": gy + sign, "gz": other},
                                device_id_type=MESH)
        total = total + jnp.where(has["gy", sign], 1, 0)
    diagonals = [(a, b) for a in (-1, 1) for b in (-1, 1)]

    def both_ways(a, b):
        return jnp.logical_and(has["gx", a], has["gy", b])

    for a, b in diagonals:
        @pl.when(both_ways(a, b))
        def _(a=a, b=b):
            pl.semaphore_signal(barrier, inc=1, device_id={"gx": gx + a, "gy": gy + b},
                                device_id_type=MESH)
        total = total + jnp.where(both_ways(a, b), 1, 0)

    own_m = pltpu.make_async_copy(mat_ref, mat, local.at[0])
    own_m.start()
    step = nx // 4
    own_v = [pltpu.make_async_copy(v_ref.at[n * step:(n + 1) * step],
                                   e.at[1 + n * step:1 + (n + 1) * step, GHOST:tail], local.at[2 + n])
             for n in range(4)]
    for copy in own_v:
        copy.start()
    own_t = pltpu.make_async_copy(t_hbm.at[gz], t, local.at[1])
    own_t.start()

    used = [0]
    sent = []

    def remote(src, dst, device, cond=None, got=None):
        n = used[0]
        used[0] += 1
        copy = pltpu.make_async_remote_copy(src_ref=src, dst_ref=dst, send_sem=send.at[n],
                                            recv_sem=recv.at[n], device_id=device,
                                            device_id_type=MESH)

        def when(test, action):
            if test is None:
                action()
            else:
                pl.when(test)(action)

        sent.append(lambda: when(cond, copy.wait_send))
        return lambda: when(cond, copy.start), lambda: when(got, copy.wait_recv)

    def shift(axis, sign, src, dst):
        return remote(src, dst, {axis: at[axis] + sign}, has[axis, sign], has[axis, -sign])

    def partner(src, dst, cond=None):
        return remote(src, dst, {"gz": other}, cond, cond)

    def zero(cond, ref):
        @pl.when(jnp.logical_not(cond))
        def _():
            ref[...] = jnp.zeros(ref.shape, ref.dtype)

    mid = slice(8, 8 + nx)
    zero(has["gx", -1], e.at[0])
    zero(has["gx", 1], e.at[nx + 1])
    zero(has["gy", -1], m.at[:, 0, mid])
    zero(top, m.at[:, ny_cells + 1, mid])
    zero(has["gx", -1], xf_in.at[1])
    zero(has["gx", 1], xf_in.at[0])
    for at_row in (0, 8 + nx):
        m[:, :, at_row:at_row + 8] = jnp.zeros((2, ny_cells + 2, 8, LANES), f32)
    for n, (a, b) in enumerate(diagonals):
        zero(both_ways(-a, -b), c_in.at[n])
    zero(top, g.at[1:nx + 1])
    zero(jnp.logical_and(top, has["gx", -1]), g.at[0])
    zero(jnp.logical_and(top, has["gx", 1]), g.at[nx + 1])
    zero(top, cz_in)
    m[:, 1:ny_cells + 1, mid] = jnp.zeros((2, ny_cells, nx, LANES), f32)
    own_m.wait()
    for f in range(2):
        for y in range(ny_cells):
            m[f, y + 1, mid, :size_z] = mat[f, :, y, :]
    first_x, last_x = 8, 7 + nx
    c_out[...] = jnp.zeros(c_out.shape, f32)
    for f in range(2):
        xf_out[0, f] = m[f, 1:ny_cells + 1, first_x, :]
        xf_out[1, f] = m[f, 1:ny_cells + 1, last_x, :]
        for n, (a, b) in enumerate(diagonals):
            x, y = first_x if a < 0 else last_x, 1 if b < 0 else ny_cells
            c_out[n, f, 0:1] = m[f, y, x:x + 1]

    pl.semaphore_wait(barrier, total)

    my_down = shift("gy", -1, m.at[:, 1, mid], m.at[:, ny_cells + 1, mid])
    my_up = shift("gy", 1, m.at[:, ny_cells, mid], m.at[:, 0, mid])
    mx_down = shift("gx", -1, xf_out.at[0], xf_in.at[0])
    mx_up = shift("gx", 1, xf_out.at[1], xf_in.at[1])
    corners = [remote(c_out.at[n], c_in.at[n], {"gx": gx + a, "gy": gy + b},
                      both_ways(a, b), both_ways(-a, -b)) for n, (a, b) in enumerate(diagonals)]
    material_copies = [my_down, my_up, mx_down, mx_up] + corners
    for copy in material_copies:
        copy[0]()
    bounds = [(nx - 1, nx), (0, 1), (1, 3)] + [(a, min(a + 4, nx - 1)) for a in range(3, nx - 1, 4)]
    y_ghosts = [shift("gy", -1, v_ref.at[a:b, :size_z], g.at[a + 1:b + 1, :size_z]) for a, b in bounds]
    for copy in y_ghosts[:3]:
        copy[0]()
    x_down = shift("gx", -1, v_ref.at[0], e.at[nx + 1, GHOST:tail])
    x_up = shift("gx", 1, v_ref.at[nx - 1], e.at[0, GHOST:tail])

    x_down[0]()
    x_up[0]()

    edge = jnp.where(gz == 0, size_z - 1, 0)
    row = lax.broadcasted_iota(jnp.int32, (GHOST, own), 0)
    col = lax.broadcasted_iota(jnp.int32, (GHOST, own), 1)
    pick = jnp.logical_and(row < ny_cells, col == row * size_z + edge)
    pick = jnp.where(pick, 1.0, 0.0).astype(bf16)

    def take_edge(x):
        zs[x] = jnp.dot(pick, e[x, GHOST:tail], preferred_element_type=f32).astype(bf16)

    z_own = []
    for n in range(4):
        own_v[n].wait()
        low, high = 1 + n * step, 1 + (n + 1) * step
        for x in range(low, high):
            take_edge(x)
        z_own.append([partner(zs.at[low:high], e.at[low:high, :GHOST]),
                      partner(zs.at[low:high], e.at[low:high, tail:])])
        for copy in z_own[n]:
            copy[0]()
    row = lax.broadcasted_iota(jnp.int32, (nx, nx * GHOST), 0)
    col = lax.broadcasted_iota(jnp.int32, (nx, nx * GHOST), 1)
    pick2 = jnp.where(col == row * GHOST, 1.0, 0.0).astype(bf16)
    cz_out[...] = jnp.dot(pick2, zs[1:nx + 1].reshape(nx * GHOST, columns),
                          preferred_element_type=f32).astype(bf16)
    corner = remote(cz_out, cz_in, {"gy": gy - 1, "gz": other}, has["gy", -1], top)
    corner[0]()
    for copy in y_ghosts[3:]:
        copy[0]()
    own_t.wait()

    ring_size = pp.shape[0]

    def ring(x):
        return pp.at[x % ring_size]

    def taps_of(x, dst, *more):
        first = jnp.dot(t[0], e[x + 1, :kw], preferred_element_type=f32)
        second = jnp.dot(t[1], e[x + 1, tail + GHOST - kw:], preferred_element_type=f32)
        for ref in (dst,) + more:
            ref[:2 * hz] = first
            ref[2 * hz:] = second

    acc[...] = jnp.zeros_like(acc)
    def arrived(n):
        for copy in z_own[n]:
            copy[1]()

    arrived(0)
    taps_of(0, ring(0), ps0)
    taps_of(1, ring(1), ps1)
    for x in range(2, step):
        taps_of(x, ring(x))
    for copy in material_copies:
        copy[1]()
    for f in range(2):
        for y in range(ny_cells):
            m[f, y + 1, last_x + 1:last_x + 2] = xf_in[0, f, y:y + 1]
            m[f, y + 1, first_x - 1:first_x] = xf_in[1, f, y:y + 1]
        for n, (a, b) in enumerate(diagonals):
            x, y = last_x + 1 if a < 0 else first_x - 1, ny_cells + 1 if b < 0 else 0
            m[f, y, x:x + 1] = c_in[n, f, 0:1]
    mz_copy = partner(m, mz)
    mz_copy[0]()
    arrived(1)
    for x in range(step, step + 2):
        taps_of(x, ring(x))
    for n in range(2, 4):
        arrived(n)
    ready = ring_size - 1
    for x in range(step + 2, ready):
        taps_of(x, ring(x))
    mz_copy[1]()

    lanes = lax.broadcasted_iota(jnp.int32, (m.shape[2], LANES), 1)
    turn = jnp.where(gz == 0, size_z - 1, LANES - size_z + 1)

    def z_sum(y):
        k = m[0, y]
        ghost = jnp.where(lanes == edge, pltpu.roll(mz[0, y], turn, 1), 0.0)
        return pltpu.roll(k, 1, 1) + 2.0 * k + pltpu.roll(k, LANES - 1, 1) + ghost

    sums = [z_sum(y) for y in range(ny_cells + 2)]
    for y in range(ny_cells):
        fy[y] = sums[y] + 2.0 * sums[y + 1] + sums[y + 2]
        field = fy[y, 7:7 + nx] + 2.0 * fy[y, 8:8 + nx] + fy[y, 9:9 + nx]
        kappa = m[0, y + 1, mid]
        rho = m[1, y + 1, mid]
        both = jnp.concatenate([2.0 * kappa + field * (1.0 / 32.0), kappa * (1.0 / 16.0),
                                rho * (1.0 / 216.0)], 0)
        cols[y, :, :3 * nx] = both.T[:size_z]

    dims = (((0,), (0,)), ((), ()))

    def column(x, y, c):
        return jnp.broadcast_to(cols[y, :, c * nx + x:c * nx + x + 1], (size_z, LANES))

    def values(xs, planes, dst, base=0):
        for y in range(ny_cells):
            h, yy = divmod(y, half)
            sr = slice(2 * hz * h + size_z * yy, 2 * hz * h + size_z * (yy + 1))
            mr = slice(sr.start + hz, sr.stop + hz)
            coef = [[column(x, y, c) for c in range(3)] for x in xs]
            for at_lane in range(0, columns, LANES):
                ll = slice(at_lane, at_lane + LANES)
                p = [ref[sr, ll] for ref in planes]
                q = [ref[mr, ll] for ref in planes]
                for k, x in enumerate(xs):
                    d, kq, rq = coef[k]
                    rr = slice(base + k * own + size_z * y, base + k * own + size_z * (y + 1))
                    v = e[x + 1, GHOST + size_z * y:GHOST + size_z * (y + 1), ll].astype(f32)
                    s = p[k] + p[k + 2] + 2.0 * p[k + 1]
                    w = q[k] + q[k + 2] + 4.0 * q[k + 1]
                    dst[rr, ll] = (d * v - kq * s).astype(bf16)
                    dst[rr, slice(columns + at_lane, columns + at_lane + LANES)] = (rq * w).astype(bf16)

    def gram(first, second, src):
        v = jnp.concatenate([e[first + 1, GHOST:tail], e[second + 1, GHOST:tail]], 0)
        acc[...] += lax.dot_general(v, src[...], dims, preferred_element_type=f32)

    def relay(sign, src, dst):
        return remote(g.at[src, :size_z], g.at[dst, :size_z], {"gx": gx + sign},
                      jnp.logical_and(top, has["gx", sign]), jnp.logical_and(top, has["gx", -sign]))

    relays = [relay(-1, 1, nx + 1), relay(1, nx, 0)]
    z_ghosts = [partner(zs.at[x], e.at[x, at_row:at_row + GHOST])
                for x in (0, nx + 1) for at_row in (0, tail)]
    zrow = pl.multiple_of(jnp.where(gz == 0, size_z - GHOST, 0), GHOST)
    z_relays = [partner(g.at[j, pl.ds(zrow, GHOST)], g.at[j, size_z:], top) for j in (0, nx + 1)]

    reach = jnp.where(gz == 0, size_z, GHOST)
    mine = lanes < size_z

    def ghost_columns(f, factor):
        k = m[f, ny_cells + 1]
        return jnp.where(mine, k, pltpu.roll(mz[f, ny_cells + 1], reach, 1)) * factor

    def prepare_ghosts():
        both = jnp.concatenate([ghost_columns(0, 1.0 / 16.0), ghost_columns(1, 1.0 / 216.0)], 0)
        ghost_cols = both.T[:group]
        for f in range(2):
            for j in range(nx + 2):
                n = f * m.shape[2] + 7 + j
                gc[f, j] = jnp.broadcast_to(ghost_cols[:, n:n + 1], (group, LANES))
        for x in range(nx):
            one = cz_in[x:x + 1].astype(f32)
            g[x + 1, size_z:] = jnp.broadcast_to(one, (GHOST, columns)).astype(bf16)

    two_z = 2 * size_z

    def weigh(j):
        for at_lane in range(0, columns, LANES):
            ll = slice(at_lane, at_lane + LANES)
            v = g[j, :, ll].astype(f32)
            gk[j, :, ll] = (v * gc[0, j]).astype(bf16)
            gr[j, :, ll] = (v * gc[1, j]).astype(bf16)

    def late(x, side):
        taps = t[2, side * two_z:(side + 1) * two_z, :4 * group]
        weighed = (gk, gr)[side]
        coef = [column(x + o, ny_cells - 1, 1 + side) for o in range(2)]
        for at_lane in range(0, columns, 2 * LANES):
            ll = slice(at_lane, at_lane + 2 * LANES)
            plain = jnp.dot(taps, g[x:x + 4, :, ll].reshape(4 * group, 2 * LANES),
                            preferred_element_type=f32)
            heavy = jnp.dot(taps, weighed[x:x + 4, :, ll].reshape(4 * group, 2 * LANES),
                            preferred_element_type=f32)
            for o in range(2):
                rr = slice(o * size_z, (o + 1) * size_z)
                c = jnp.concatenate([coef[o]] * 2, 1)
                if side == 0:
                    value = (-c) * plain[rr] - heavy[rr]
                else:
                    value = c * plain[rr] + heavy[rr]
                yl[side, x + o, :, ll] = value.astype(bf16)

    def late_gram(first, stop, side):
        v = jnp.concatenate([e[x + 1, tail - size_z:tail] for x in range(first, stop)], 0)
        y = yl[side, first:stop].reshape((stop - first) * size_z, columns)
        ll = slice(side * columns, (side + 1) * columns)
        acc[:, ll] += lax.dot_general(v, y, dims, preferred_element_type=f32)

    def stage(n):
        if n == 3:
            for copy in y_ghosts[:2]:
                copy[1]()
            for copy in relays:
                copy[0]()
        elif n == 5:
            x_down[1]()
            x_up[1]()
            take_edge(0)
            take_edge(nx + 1)
            for copy in z_ghosts:
                copy[0]()
            for copy in relays:
                copy[1]()
            for copy in z_relays:
                copy[0]()
        elif n == 6:
            for copy in z_ghosts:
                copy[1]()
            corner[1]()
        elif n == 7:
            for copy in z_relays:
                copy[1]()
            for copy in y_ghosts[2:5]:
                copy[1]()

    pairs = [(x, x + 1) for x in range(1, nx - 1, 2)] + [(nx - 1, 0)]
    previous = None
    for n, pair in enumerate(pairs):
        stage(n)
        y_now = (ya, yb)[n % 2]
        if pair[1]:
            values(pair, [ring(x) for x in range(pair[0] - 1, pair[1] + 2)], y_now)
        else:
            values((nx - 1,), [ring(nx - 2), ring(nx - 1), ring(nx)], y_now)
            values((0,), [ring(nx + 1), ps0, ps1], y_now, own)
        for x in (ready + 2 * n, ready + 2 * n + 1):
            if x < nx:
                taps_of(x, ring(x))
        if n == 6:
            taps_of(nx, ring(nx))
            taps_of(-1, ring(nx + 1))
        if n == 6:
            prepare_ghosts()
        if previous is not None:
            gram(*previous)
        previous = pair + (y_now,)
    soon = nx - 6
    for j in list(range(soon + 2)) + [nx, nx + 1]:
        weigh(j)
    for side in range(2):
        for x in range(0, soon, 2):
            late(x, side)
    gram(*previous)
    for side in range(2):
        late_gram(0, soon, side)
    y_ghosts[5][1]()
    for j in range(soon + 2, nx):
        weigh(j)

    def finish(side):
        for x in range(soon, nx, 2):
            late(x, side)
        late_gram(soon, nx, side)

    rows = out_ref.shape[0]

    def symmetric(side):
        ll = slice(side * columns, (side + 1) * columns)
        a = acc[:, ll]
        a = (a + a.T) * scale
        for n in range(columns // rows):
            i, rest = divmod(n, cy * cz)
            j, k = divmod(rest, cz)
            part[i, j, k, :, ll] = a[n * rows:(n + 1) * rows]

    def everywhere(axis, piece, landing):
        count = lax.axis_size(axis)
        me = lax.axis_index(axis)
        copies = []
        for k in range(1, count):
            peer = lax.rem(me + k, count)
            copy = remote(piece(peer), landing.at[k - 1], {axis: peer})
            copy[0]()
            copies.append(copy)
        return copies

    def collect(copies, held, landing):
        for copy in copies:
            copy[1]()
        for k in range(len(copies)):
            held = held + landing[k]
        return held

    flights = [None] * len(chunks)

    def leave(n):
        lo, hi, by = chunks[n]
        flights[n] = everywhere("gz", lambda p: part.at[:, :, p, :, lo:hi], buffers[n][0])

    def first_round(n):
        lo, hi, by = chunks[n]
        rz, s1, r1, s2, r2 = buffers[n]
        s1[...] = collect(flights[n], part[:, :, gz, :, lo:hi], rz)
        if by == "gy":
            flights[n] = everywhere("gy", lambda p: s1.at[:, p], r1)
        else:
            flights[n] = everywhere("gx", lambda p: s1.at[p], r1)

    halves = [[n for n, c in enumerate(chunks) if c[0] // columns == side] for side in range(2)]
    finish(0)
    symmetric(0)
    for n in halves[0]:
        leave(n)
    finish(1)
    for n in halves[0]:
        first_round(n)
    symmetric(1)
    for n in halves[1]:
        leave(n)
    for n in halves[1]:
        first_round(n)
    for n, (lo, hi, by) in enumerate(chunks):
        rz, s1, r1, s2, r2 = buffers[n]
        mine_now = s1[:, gy] if by == "gy" else s1[gx]
        s2[...] = collect(flights[n], mine_now, r1)
        flights[n] = everywhere("gx" if by == "gy" else "gy", lambda p, s2=s2: s2.at[p], r2)
    for n, (lo, hi, by) in enumerate(chunks):
        rz, s1, r1, s2, r2 = buffers[n]
        out_ref[:, lo:hi] = collect(flights[n], s2[gx] if by == "gy" else s2[gy], r2)
    for done in sent:
        done()


def per_device(eigvecs, material):
    size_x, size_y, size_z, columns = eigvecs.shape
    nx, ny, nz = (lax.axis_size(a) for a in ("gx", "gy", "gz"))
    total_cells = size_x * size_y * size_z * nx * ny * nz
    own = size_y * size_z
    tail = own + 2 * GHOST
    group = size_z + GHOST
    rows = columns // (nx * ny * nz)
    wide = 2 * columns
    matrices = jnp.asarray(tap_matrices(size_y, size_z), jnp.bfloat16)
    parts = ((2, "gy"), (2, "gx"), (2, "gy"), (1, "gy"), (1, "gy"))
    unit = wide // 8
    chunks, lo = [], 0
    for width, by in parts:
        chunks.append((lo, lo + width * unit, by))
        lo += width * unit
    f32, bf16 = jnp.float32, jnp.bfloat16
    dma = pltpu.SemaphoreType.DMA
    vmem = pl.BlockSpec(memory_space=pltpu.VMEM)
    anywhere = pl.BlockSpec(memory_space=pl.ANY)
    copies = 56 + len(chunks) * (nx + ny + nz - 3)
    plane = ((2 * own, columns), f32)
    face, corner = ((2, 2, size_y, LANES), f32), ((4, 2, 8, LANES), f32)
    scratch = [
        (material.shape, f32), face, face, corner, corner,
        ((size_x + 2, tail, columns), bf16),
        ((12, 2 * own, columns), f32), plane, plane,
        ((2 * own, wide), bf16), ((2 * own, wide), bf16),
        ((columns, wide), f32),
        (matrices.shape[1:], bf16),
        ((size_x + 2, GHOST, columns), bf16),
        ((size_x, columns), bf16),
        ((size_x, columns), bf16),
        ((2, size_y + 2, size_x + 16, LANES), f32),
        ((2, size_y + 2, size_x + 16, LANES), f32),
        ((size_y, size_x + 16, LANES), f32),
        ((size_y, size_z, LANES), f32),
        ((2, size_x + 2, group, LANES), f32),
        ((size_x + 2, group, columns), bf16),
        ((size_x + 2, group, columns), bf16),
        ((size_x + 2, group, columns), bf16),
        ((2, size_x, size_z, columns), bf16),
        ((nx, ny, nz, rows, wide), f32),
    ]
    for low, high, by in chunks:
        w = high - low
        n1, n2 = (ny, nx) if by == "gy" else (nx, ny)
        scratch += [((nz - 1, nx, ny, rows, w), f32), ((nx, ny, rows, w), f32),
                    ((n1 - 1, n2, rows, w), f32), ((n2, rows, w), f32), ((n2 - 1, rows, w), f32)]
    out = pl.pallas_call(
        functools.partial(kernel, 0.5 / total_cells, tuple(chunks)),
        out_shape=jax.ShapeDtypeStruct((rows, wide), f32),
        in_specs=[anywhere] * 3,
        out_specs=vmem,
        scratch_shapes=[pltpu.VMEM(*s) for s in scratch] + [dma((6,)), dma((copies,)), dma((copies,))],
        compiler_params=pltpu.CompilerParams(
            vmem_limit_bytes=63 * 1024 * 1024, collective_id=0, has_side_effects=True),
    )(eigvecs.reshape(size_x, own, columns), material, matrices)
    return out[:, :columns], out[:, columns:]


def solution(mesh):
    return jax.shard_map(
        per_device,
        mesh=mesh,
        in_specs=(P("gx", "gy", "gz", None), P(None, "gx", "gy", "gz")),
        out_specs=(P(("gx", "gy", "gz"), None), P(("gx", "gy", "gz"), None)),
        check_vma=False,
    )
```

```python
import functools
import numpy as np
import jax
import jax.numpy as jnp
from jax import lax
from jax.experimental import pallas as pl
from jax.experimental.pallas import tpu as pltpu
from jax.sharding import PartitionSpec as P

LANES = 128
GHOST = 16
MESH = pl.DeviceIdType.MESH
AXES = ("gx", "gy", "gz")


def tap(a, b, middle):
    return middle if a == b else (1.0 if abs(a - b) == 1 else 0.0)


def tap_matrices(size_y, size_z):
    half = size_y // 2
    width = (half + 1) * size_z + GHOST
    sides = []
    for side in (0, 1):
        edge = size_z - 1 if side == 0 else 0
        blocks = []
        for first in (0, 1):
            ys_in = range(0, half + 1) if first == 0 else range(half - 1, size_y)
            ys_out = range(0, half) if first == 0 else range(half, size_y)
            own_at = GHOST if first == 0 else 0
            ghost_at = 0 if first == 0 else (half + 1) * size_z
            rows = []
            for middle in (2.0, 4.0):
                zz = middle * np.eye(size_z) + np.eye(size_z, k=1) + np.eye(size_z, k=-1)
                block = np.zeros((half * size_z, width))
                for o, y in enumerate(ys_out):
                    for n, y2 in enumerate(ys_in):
                        w = tap(y, y2, middle)
                        if w:
                            block[o * size_z:(o + 1) * size_z,
                                  own_at + n * size_z:own_at + (n + 1) * size_z] = w * zz
                            block[o * size_z + edge, ghost_at + y2] = w
                rows.append(block)
            blocks.append(np.concatenate(rows, 0))
        group = size_z + GHOST
        rows = []
        for middle in (2.0, 4.0):
            one = np.zeros((size_z, group))
            one[:, :size_z] = middle * np.eye(size_z) + np.eye(size_z, k=1) + np.eye(size_z, k=-1)
            one[edge, size_z + (0 if side == 0 else GHOST - 1)] = 1.0
            along = np.array([[tap(o + 1, j, middle) for j in range(4)] for o in range(2)])
            rows.append(np.kron(along, one))
        late = np.concatenate(rows, 0)
        full = np.zeros((blocks[0].shape[0], width))
        full[:late.shape[0], :late.shape[1]] = late
        blocks.append(full)
        sides.append(np.stack(blocks))
    return np.stack(sides)


def kernel(scale, chunks, v_ref, mat_ref, t_hbm, out_ref,
           mat, xf_out, xf_in, c_out, c_in, e, pp, ps0, ps1, ya, yb, acc, t, zs, cz_out, cz_in, m, mz, fy, cols, gc, g, gk, gr, yl,
           part, *rest):
    f32, bf16 = jnp.float32, jnp.bfloat16
    local, send, recv = rest[-3:]
    buffers = [rest[5 * n:5 * n + 5] for n in range(len(chunks))]
    nx, own, columns = v_ref.shape
    ny_cells, size_z = mat.shape[2:]
    half = ny_cells // 2
    group = size_z + GHOST
    hz = half * size_z
    kw = t.shape[2]
    tail = GHOST + own
    gx, gy, gz = (lax.axis_index(a) for a in AXES)
    cx, cy, cz = (lax.axis_size(a) for a in AXES)
    has = {("gx", -1): gx > 0, ("gx", 1): gx < cx - 1, ("gy", -1): gy > 0, ("gy", 1): gy < cy - 1}
    at = {"gx": gx, "gy": gy}
    top = has["gy", 1]
    other = lax.rem(gz + 1, cz)
    barrier = pltpu.get_barrier_semaphore()
    total = 0
    for axis, count in (("gz", cz), ("gy", cy), ("gx", cx)):
        me = lax.axis_index(axis)
        for k in range(1, count):
            pl.semaphore_signal(barrier, inc=1, device_id={axis: lax.rem(me + k, count)},
                                device_id_type=MESH)
        total += count - 1
    for sign in (-1, 1):
        @pl.when(has["gy", sign])
        def _(sign=sign):
            pl.semaphore_signal(barrier, inc=1, device_id={"gy": gy + sign, "gz": other},
                                device_id_type=MESH)
        total = total + jnp.where(has["gy", sign], 1, 0)
    diagonals = [(a, b) for a in (-1, 1) for b in (-1, 1)]

    def both_ways(a, b):
        return jnp.logical_and(has["gx", a], has["gy", b])

    for a, b in diagonals:
        @pl.when(both_ways(a, b))
        def _(a=a, b=b):
            pl.semaphore_signal(barrier, inc=1, device_id={"gx": gx + a, "gy": gy + b},
                                device_id_type=MESH)
        total = total + jnp.where(both_ways(a, b), 1, 0)

    own_m = pltpu.make_async_copy(mat_ref, mat, local.at[0])
    own_m.start()
    step = nx // 4
    own_v = [pltpu.make_async_copy(v_ref.at[n * step:(n + 1) * step],
                                   e.at[1 + n * step:1 + (n + 1) * step, GHOST:tail], local.at[2 + n])
             for n in range(4)]
    for copy in own_v:
        copy.start()
    own_t = pltpu.make_async_copy(t_hbm.at[gz], t, local.at[1])
    own_t.start()

    used = [0]
    sent = []

    def remote(src, dst, device, cond=None, got=None):
        n = used[0]
        used[0] += 1
        copy = pltpu.make_async_remote_copy(src_ref=src, dst_ref=dst, send_sem=send.at[n],
                                            recv_sem=recv.at[n], device_id=device,
                                            device_id_type=MESH)

        def when(test, action):
            if test is None:
                action()
            else:
                pl.when(test)(action)

        sent.append(lambda: when(cond, copy.wait_send))
        return lambda: when(cond, copy.start), lambda: when(got, copy.wait_recv)

    def shift(axis, sign, src, dst):
        return remote(src, dst, {axis: at[axis] + sign}, has[axis, sign], has[axis, -sign])

    def partner(src, dst, cond=None):
        return remote(src, dst, {"gz": other}, cond, cond)

    def zero(cond, ref):
        @pl.when(jnp.logical_not(cond))
        def _():
            ref[...] = jnp.zeros(ref.shape, ref.dtype)

    mid = slice(8, 8 + nx)
    zero(has["gx", -1], e.at[0])
    zero(has["gx", 1], e.at[nx + 1])
    zero(has["gy", -1], m.at[:, 0, mid])
    zero(top, m.at[:, ny_cells + 1, mid])
    zero(has["gx", -1], xf_in.at[1])
    zero(has["gx", 1], xf_in.at[0])
    for at_row in (0, 8 + nx):
        m[:, :, at_row:at_row + 8] = jnp.zeros((2, ny_cells + 2, 8, LANES), f32)
    for n, (a, b) in enumerate(diagonals):
        zero(both_ways(-a, -b), c_in.at[n])
    zero(top, g.at[1:nx + 1])
    zero(jnp.logical_and(top, has["gx", -1]), g.at[0])
    zero(jnp.logical_and(top, has["gx", 1]), g.at[nx + 1])
    zero(top, cz_in)
    m[:, 1:ny_cells + 1, mid] = jnp.zeros((2, ny_cells, nx, LANES), f32)
    own_m.wait()
    for f in range(2):
        for y in range(ny_cells):
            m[f, y + 1, mid, :size_z] = mat[f, :, y, :]
    first_x, last_x = 8, 7 + nx
    c_out[...] = jnp.zeros(c_out.shape, f32)
    for f in range(2):
        xf_out[0, f] = m[f, 1:ny_cells + 1, first_x, :]
        xf_out[1, f] = m[f, 1:ny_cells + 1, last_x, :]
        for n, (a, b) in enumerate(diagonals):
            x, y = first_x if a < 0 else last_x, 1 if b < 0 else ny_cells
            c_out[n, f, 0:1] = m[f, y, x:x + 1]

    pl.semaphore_wait(barrier, total)

    my_down = shift("gy", -1, m.at[:, 1, mid], m.at[:, ny_cells + 1, mid])
    my_up = shift("gy", 1, m.at[:, ny_cells, mid], m.at[:, 0, mid])
    mx_down = shift("gx", -1, xf_out.at[0], xf_in.at[0])
    mx_up = shift("gx", 1, xf_out.at[1], xf_in.at[1])
    corners = [remote(c_out.at[n], c_in.at[n], {"gx": gx + a, "gy": gy + b},
                      both_ways(a, b), both_ways(-a, -b)) for n, (a, b) in enumerate(diagonals)]
    material_copies = [my_down, my_up, mx_down, mx_up] + corners
    for copy in material_copies:
        copy[0]()
    bounds = [(nx - 1, nx), (0, 1), (1, 3), (3, 7), (7, nx - 5), (nx - 5, nx - 3), (nx - 3, nx - 1)]
    y_ghosts = [shift("gy", -1, v_ref.at[a:b, :size_z], g.at[a + 1:b + 1, :size_z]) for a, b in bounds]
    for copy in y_ghosts[:3]:
        copy[0]()
    x_down = shift("gx", -1, v_ref.at[0], e.at[nx + 1, GHOST:tail])
    x_up = shift("gx", 1, v_ref.at[nx - 1], e.at[0, GHOST:tail])

    x_down[0]()
    x_up[0]()

    edge = jnp.where(gz == 0, size_z - 1, 0)
    row = lax.broadcasted_iota(jnp.int32, (GHOST, own), 0)
    col = lax.broadcasted_iota(jnp.int32, (GHOST, own), 1)
    pick = jnp.logical_and(row < ny_cells, col == row * size_z + edge)
    pick = jnp.where(pick, 1.0, 0.0).astype(bf16)

    def take_edge(x):
        zs[x] = jnp.dot(pick, e[x, GHOST:tail], preferred_element_type=f32).astype(bf16)

    z_own = []
    for n in range(4):
        own_v[n].wait()
        low, high = 1 + n * step, 1 + (n + 1) * step
        for x in range(low, high):
            take_edge(x)
        z_own.append([partner(zs.at[low:high], e.at[low:high, :GHOST]),
                      partner(zs.at[low:high], e.at[low:high, tail:])])
        for copy in z_own[n]:
            copy[0]()
    row = lax.broadcasted_iota(jnp.int32, (nx, nx * GHOST), 0)
    col = lax.broadcasted_iota(jnp.int32, (nx, nx * GHOST), 1)
    pick2 = jnp.where(col == row * GHOST, 1.0, 0.0).astype(bf16)
    cz_out[...] = jnp.dot(pick2, zs[1:nx + 1].reshape(nx * GHOST, columns),
                          preferred_element_type=f32).astype(bf16)
    corner = remote(cz_out, cz_in, {"gy": gy - 1, "gz": other}, has["gy", -1], top)
    corner[0]()
    for copy in y_ghosts[3:]:
        copy[0]()
    own_t.wait()

    ring_size = pp.shape[0]

    def ring(x):
        return pp.at[x % ring_size]

    def taps_of(x, dst, *more):
        first = jnp.dot(t[0], e[x + 1, :kw], preferred_element_type=f32)
        second = jnp.dot(t[1], e[x + 1, tail + GHOST - kw:], preferred_element_type=f32)
        for ref in (dst,) + more:
            ref[:2 * hz] = first
            ref[2 * hz:] = second

    acc[...] = jnp.zeros_like(acc)
    def arrived(n):
        for copy in z_own[n]:
            copy[1]()

    arrived(0)
    taps_of(0, ring(0), ps0)
    taps_of(1, ring(1), ps1)
    for x in range(2, step):
        taps_of(x, ring(x))
    for copy in material_copies:
        copy[1]()
    for f in range(2):
        for y in range(ny_cells):
            m[f, y + 1, last_x + 1:last_x + 2] = xf_in[0, f, y:y + 1]
            m[f, y + 1, first_x - 1:first_x] = xf_in[1, f, y:y + 1]
        for n, (a, b) in enumerate(diagonals):
            x, y = last_x + 1 if a < 0 else first_x - 1, ny_cells + 1 if b < 0 else 0
            m[f, y, x:x + 1] = c_in[n, f, 0:1]
    mz_copy = partner(m, mz)
    mz_copy[0]()
    arrived(1)
    for x in range(step, step + 2):
        taps_of(x, ring(x))
    for n in range(2, 4):
        arrived(n)
    ready = ring_size - 1
    for x in range(step + 2, ready):
        taps_of(x, ring(x))
    mz_copy[1]()

    lanes = lax.broadcasted_iota(jnp.int32, (m.shape[2], LANES), 1)
    turn = jnp.where(gz == 0, size_z - 1, LANES - size_z + 1)

    def z_sum(y):
        k = m[0, y]
        ghost = jnp.where(lanes == edge, pltpu.roll(mz[0, y], turn, 1), 0.0)
        return pltpu.roll(k, 1, 1) + 2.0 * k + pltpu.roll(k, LANES - 1, 1) + ghost

    sums = [z_sum(y) for y in range(ny_cells + 2)]
    for y in range(ny_cells):
        fy[y] = sums[y] + 2.0 * sums[y + 1] + sums[y + 2]
        field = fy[y, 7:7 + nx] + 2.0 * fy[y, 8:8 + nx] + fy[y, 9:9 + nx]
        kappa = m[0, y + 1, mid]
        rho = m[1, y + 1, mid]
        both = jnp.concatenate([2.0 * kappa + field * (1.0 / 32.0), kappa * (1.0 / 16.0),
                                rho * (1.0 / 216.0)], 0)
        cols[y, :, :3 * nx] = both.T[:size_z]

    dims = (((0,), (0,)), ((), ()))

    def column(x, y, c):
        return jnp.broadcast_to(cols[y, :, c * nx + x:c * nx + x + 1], (size_z, LANES))

    def values(xs, planes, dst, base=0):
        for y in range(ny_cells):
            h, yy = divmod(y, half)
            sr = slice(2 * hz * h + size_z * yy, 2 * hz * h + size_z * (yy + 1))
            mr = slice(sr.start + hz, sr.stop + hz)
            coef = [[column(x, y, c) for c in range(3)] for x in xs]
            for at_lane in range(0, columns, LANES):
                ll = slice(at_lane, at_lane + LANES)
                p = [ref[sr, ll] for ref in planes]
                q = [ref[mr, ll] for ref in planes]
                for k, x in enumerate(xs):
                    d, kq, rq = coef[k]
                    rr = slice(base + k * own + size_z * y, base + k * own + size_z * (y + 1))
                    v = e[x + 1, GHOST + size_z * y:GHOST + size_z * (y + 1), ll].astype(f32)
                    s = p[k] + p[k + 2] + 2.0 * p[k + 1]
                    w = q[k] + q[k + 2] + 4.0 * q[k + 1]
                    dst[rr, ll] = (d * v - kq * s).astype(bf16)
                    dst[rr, slice(columns + at_lane, columns + at_lane + LANES)] = (rq * w).astype(bf16)

    def gram(first, second, src):
        v = jnp.concatenate([e[first + 1, GHOST:tail], e[second + 1, GHOST:tail]], 0)
        acc[...] += lax.dot_general(v, src[...], dims, preferred_element_type=f32)

    def relay(sign, src, dst):
        return remote(g.at[src, :size_z], g.at[dst, :size_z], {"gx": gx + sign},
                      jnp.logical_and(top, has["gx", sign]), jnp.logical_and(top, has["gx", -sign]))

    relays = [relay(-1, 1, nx + 1), relay(1, nx, 0)]
    z_ghosts = [partner(zs.at[x], e.at[x, at_row:at_row + GHOST])
                for x in (0, nx + 1) for at_row in (0, tail)]
    zrow = pl.multiple_of(jnp.where(gz == 0, size_z - GHOST, 0), GHOST)
    z_relays = [partner(g.at[j, pl.ds(zrow, GHOST)], g.at[j, size_z:], top) for j in (0, nx + 1)]

    reach = jnp.where(gz == 0, size_z, GHOST)
    mine = lanes < size_z

    def ghost_columns(f, factor):
        k = m[f, ny_cells + 1]
        return jnp.where(mine, k, pltpu.roll(mz[f, ny_cells + 1], reach, 1)) * factor

    def prepare_ghosts():
        both = jnp.concatenate([ghost_columns(0, 1.0 / 16.0), ghost_columns(1, 1.0 / 216.0)], 0)
        ghost_cols = both.T[:group]
        for f in range(2):
            for j in range(nx + 2):
                n = f * m.shape[2] + 7 + j
                gc[f, j] = jnp.broadcast_to(ghost_cols[:, n:n + 1], (group, LANES))
        for x in range(nx):
            one = cz_in[x:x + 1].astype(f32)
            g[x + 1, size_z:] = jnp.broadcast_to(one, (GHOST, columns)).astype(bf16)

    two_z = 2 * size_z

    def weigh(j):
        for at_lane in range(0, columns, LANES):
            ll = slice(at_lane, at_lane + LANES)
            v = g[j, :, ll].astype(f32)
            gk[j, :, ll] = (v * gc[0, j]).astype(bf16)
            gr[j, :, ll] = (v * gc[1, j]).astype(bf16)

    def late(x, side):
        taps = t[2, side * two_z:(side + 1) * two_z, :4 * group]
        weighed = (gk, gr)[side]
        coef = [column(x + o, ny_cells - 1, 1 + side) for o in range(2)]
        for at_lane in range(0, columns, 2 * LANES):
            ll = slice(at_lane, at_lane + 2 * LANES)
            plain = jnp.dot(taps, g[x:x + 4, :, ll].reshape(4 * group, 2 * LANES),
                            preferred_element_type=f32)
            heavy = jnp.dot(taps, weighed[x:x + 4, :, ll].reshape(4 * group, 2 * LANES),
                            preferred_element_type=f32)
            for o in range(2):
                rr = slice(o * size_z, (o + 1) * size_z)
                c = jnp.concatenate([coef[o]] * 2, 1)
                if side == 0:
                    value = (-c) * plain[rr] - heavy[rr]
                else:
                    value = c * plain[rr] + heavy[rr]
                yl[side, x + o, :, ll] = value.astype(bf16)

    def late_gram(first, stop, side):
        v = jnp.concatenate([e[x + 1, tail - size_z:tail] for x in range(first, stop)], 0)
        y = yl[side, first:stop].reshape((stop - first) * size_z, columns)
        ll = slice(side * columns, (side + 1) * columns)
        acc[:, ll] += lax.dot_general(v, y, dims, preferred_element_type=f32)

    def stage(n):
        if n == 3:
            for copy in y_ghosts[:2]:
                copy[1]()
            for copy in relays:
                copy[0]()
        elif n == 5:
            x_down[1]()
            x_up[1]()
            take_edge(0)
            take_edge(nx + 1)
            for copy in z_ghosts:
                copy[0]()
            for copy in relays:
                copy[1]()
            for copy in z_relays:
                copy[0]()
        elif n == 6:
            for copy in z_ghosts:
                copy[1]()
            corner[1]()
        elif n == 7:
            for copy in z_relays:
                copy[1]()
            for copy in y_ghosts[2:5]:
                copy[1]()

    pairs = [(x, x + 1) for x in range(1, nx - 1, 2)] + [(nx - 1, 0)]
    previous = None
    for n, pair in enumerate(pairs):
        stage(n)
        y_now = (ya, yb)[n % 2]
        if pair[1]:
            values(pair, [ring(x) for x in range(pair[0] - 1, pair[1] + 2)], y_now)
        else:
            values((nx - 1,), [ring(nx - 2), ring(nx - 1), ring(nx)], y_now)
            values((0,), [ring(nx + 1), ps0, ps1], y_now, own)
        for x in (ready + 2 * n, ready + 2 * n + 1):
            if x < nx:
                taps_of(x, ring(x))
        if n == 6:
            taps_of(nx, ring(nx))
            taps_of(-1, ring(nx + 1))
        if n == 6:
            prepare_ghosts()
        if previous is not None:
            gram(*previous)
        previous = pair + (y_now,)
    soon = nx - 6
    for j in list(range(soon + 2)) + [nx, nx + 1]:
        weigh(j)
    for side in range(2):
        for x in range(0, soon, 2):
            late(x, side)
    gram(*previous)
    for side in range(2):
        late_gram(0, soon, side)
    y_ghosts[5][1]()
    for j in range(soon + 2, soon + 4):
        weigh(j)
    for side in range(2):
        late(soon, side)
    y_ghosts[6][1]()
    for j in range(soon + 4, nx):
        weigh(j)

    def finish(side):
        for x in range(soon + 2, nx, 2):
            late(x, side)
        late_gram(soon, nx, side)

    rows = out_ref.shape[0]

    def symmetric(side):
        ll = slice(side * columns, (side + 1) * columns)
        a = acc[:, ll]
        a = (a + a.T) * scale
        for n in range(columns // rows):
            i, rest = divmod(n, cy * cz)
            j, k = divmod(rest, cz)
            part[i, j, k, :, ll] = a[n * rows:(n + 1) * rows]

    def everywhere(axis, piece, landing):
        count = lax.axis_size(axis)
        me = lax.axis_index(axis)
        n = used[0]
        used[0] += 1

        def copy(src, dst, peer):
            return pltpu.make_async_remote_copy(src_ref=src, dst_ref=dst, send_sem=send.at[n],
                                                recv_sem=recv.at[n], device_id={axis: peer},
                                                device_id_type=MESH)

        for k in range(1, count):
            peer = lax.rem(me + k, count)
            copy(piece(peer), landing.at[k - 1], peer).start()
        whole = copy(landing, landing, lax.rem(me + 1, count))
        sent.append(whole.wait_send)
        return whole.wait_recv

    def collect(arrive, held, landing):
        arrive()
        for k in range(landing.shape[0]):
            held = held + landing[k]
        return held

    flights = [None] * len(chunks)

    def leave(n):
        lo, hi, by = chunks[n]
        flights[n] = everywhere("gz", lambda p: part.at[:, :, p, :, lo:hi], buffers[n][0])

    def first_round(n):
        lo, hi, by = chunks[n]
        rz, s1, r1, s2, r2 = buffers[n]
        s1[...] = collect(flights[n], part[:, :, gz, :, lo:hi], rz)
        if by == "gy":
            flights[n] = everywhere("gy", lambda p: s1.at[:, p], r1)
        else:
            flights[n] = everywhere("gx", lambda p: s1.at[p], r1)

    halves = [[n for n, c in enumerate(chunks) if c[0] // columns == side] for side in range(2)]
    finish(0)
    symmetric(0)
    for n in halves[0]:
        leave(n)
    finish(1)
    for n in halves[0]:
        first_round(n)
    symmetric(1)
    for n in halves[1]:
        leave(n)
    for n in halves[1]:
        first_round(n)
    for n, (lo, hi, by) in enumerate(chunks):
        rz, s1, r1, s2, r2 = buffers[n]
        mine_now = s1[:, gy] if by == "gy" else s1[gx]
        s2[...] = collect(flights[n], mine_now, r1)
        flights[n] = everywhere("gx" if by == "gy" else "gy", lambda p, s2=s2: s2.at[p], r2)
    for n, (lo, hi, by) in enumerate(chunks):
        rz, s1, r1, s2, r2 = buffers[n]
        out_ref[:, lo:hi] = collect(flights[n], s2[gx] if by == "gy" else s2[gy], r2)
    for done in sent:
        done()


def per_device(eigvecs, material):
    size_x, size_y, size_z, columns = eigvecs.shape
    nx, ny, nz = (lax.axis_size(a) for a in ("gx", "gy", "gz"))
    total_cells = size_x * size_y * size_z * nx * ny * nz
    own = size_y * size_z
    tail = own + 2 * GHOST
    group = size_z + GHOST
    rows = columns // (nx * ny * nz)
    wide = 2 * columns
    matrices = jnp.asarray(tap_matrices(size_y, size_z), jnp.bfloat16)
    parts = ((2, "gy"), (2, "gx"), (2, "gy"), (1, "gy"), (1, "gy"))
    unit = wide // 8
    chunks, lo = [], 0
    for width, by in parts:
        chunks.append((lo, lo + width * unit, by))
        lo += width * unit
    f32, bf16 = jnp.float32, jnp.bfloat16
    dma = pltpu.SemaphoreType.DMA
    vmem = pl.BlockSpec(memory_space=pltpu.VMEM)
    anywhere = pl.BlockSpec(memory_space=pl.ANY)
    copies = 35 + len(chunks) * 3
    plane = ((2 * own, columns), f32)
    face, corner = ((2, 2, size_y, LANES), f32), ((4, 2, 8, LANES), f32)
    scratch = [
        (material.shape, f32), face, face, corner, corner,
        ((size_x + 2, tail, columns), bf16),
        ((12, 2 * own, columns), f32), plane, plane,
        ((2 * own, wide), bf16), ((2 * own, wide), bf16),
        ((columns, wide), f32),
        (matrices.shape[1:], bf16),
        ((size_x + 2, GHOST, columns), bf16),
        ((size_x, columns), bf16),
        ((size_x, columns), bf16),
        ((2, size_y + 2, size_x + 16, LANES), f32),
        ((2, size_y + 2, size_x + 16, LANES), f32),
        ((size_y, size_x + 16, LANES), f32),
        ((size_y, size_z, LANES), f32),
        ((2, size_x + 2, group, LANES), f32),
        ((size_x + 2, group, columns), bf16),
        ((size_x + 2, group, columns), bf16),
        ((size_x + 2, group, columns), bf16),
        ((2, size_x, size_z, columns), bf16),
        ((nx, ny, nz, rows, wide), f32),
    ]
    for low, high, by in chunks:
        w = high - low
        n1, n2 = (ny, nx) if by == "gy" else (nx, ny)
        scratch += [((nz - 1, nx, ny, rows, w), f32), ((nx, ny, rows, w), f32),
                    ((n1 - 1, n2, rows, w), f32), ((n2, rows, w), f32), ((n2 - 1, rows, w), f32)]
    out = pl.pallas_call(
        functools.partial(kernel, 0.5 / total_cells, tuple(chunks)),
        out_shape=pltpu.VMEM((rows, wide), f32),
        in_specs=[anywhere] * 3,
        out_specs=vmem,
        scratch_shapes=[pltpu.VMEM(*s) for s in scratch] + [dma((6,)), dma((copies,)), dma((copies,))],
        compiler_params=pltpu.CompilerParams(
            vmem_limit_bytes=63 * 1024 * 1024, collective_id=0, has_side_effects=True),
    )(eigvecs.reshape(size_x, own, columns), material, matrices)
    return out[:, :columns], out[:, columns:]


def solution(mesh):
    return jax.shard_map(
        per_device,
        mesh=mesh,
        in_specs=(P("gx", "gy", "gz", None), P(None, "gx", "gy", "gz")),
        out_specs=(P(("gx", "gy", "gz"), None), P(("gx", "gy", "gz"), None)),
        check_vma=False,
    )
```

```python
import functools
import numpy as np
import jax
import jax.numpy as jnp
from jax import lax
from jax.experimental import pallas as pl
from jax.experimental.pallas import tpu as pltpu
from jax.sharding import PartitionSpec as P

LANES = 128
GHOST = 16
MESH = pl.DeviceIdType.MESH
AXES = ("gx", "gy", "gz")


def tap(a, b, middle):
    return middle if a == b else (1.0 if abs(a - b) == 1 else 0.0)


def tap_matrices(size_y, size_z):
    half = size_y // 2
    width = (half + 1) * size_z + GHOST
    sides = []
    for side in (0, 1):
        edge = size_z - 1 if side == 0 else 0
        blocks = []
        for first in (0, 1):
            ys_in = range(0, half + 1) if first == 0 else range(half - 1, size_y)
            ys_out = range(0, half) if first == 0 else range(half, size_y)
            own_at = GHOST if first == 0 else 0
            ghost_at = 0 if first == 0 else (half + 1) * size_z
            rows = []
            for middle in (2.0, 4.0):
                zz = middle * np.eye(size_z) + np.eye(size_z, k=1) + np.eye(size_z, k=-1)
                block = np.zeros((half * size_z, width))
                for o, y in enumerate(ys_out):
                    for n, y2 in enumerate(ys_in):
                        w = tap(y, y2, middle)
                        if w:
                            block[o * size_z:(o + 1) * size_z,
                                  own_at + n * size_z:own_at + (n + 1) * size_z] = w * zz
                            block[o * size_z + edge, ghost_at + y2] = w
                rows.append(block)
            blocks.append(np.concatenate(rows, 0))
        group = size_z + GHOST
        rows = []
        for middle in (2.0, 4.0):
            one = np.zeros((size_z, group))
            one[:, :size_z] = middle * np.eye(size_z) + np.eye(size_z, k=1) + np.eye(size_z, k=-1)
            one[edge, size_z + (0 if side == 0 else GHOST - 1)] = 1.0
            along = np.array([[tap(o + 1, j, middle) for j in range(4)] for o in range(2)])
            rows.append(np.kron(along, one))
        late = np.concatenate(rows, 0)
        full = np.zeros((blocks[0].shape[0], width))
        full[:late.shape[0], :late.shape[1]] = late
        blocks.append(full)
        sides.append(np.stack(blocks))
    return np.stack(sides)


def kernel(scale, chunks, v_ref, mat_ref, t_hbm, out_ref,
           mat, xf_out, xf_in, c_out, c_in, e, pp, ps0, ps1, ya, yb, acc, t, zs, cz_out, cz_in, m, mz, fy, cols, gc, g, gk, gr, yl,
           part, *rest):
    f32, bf16 = jnp.float32, jnp.bfloat16
    local, send, recv = rest[-3:]
    buffers = [rest[5 * n:5 * n + 5] for n in range(len(chunks))]
    nx, own, columns = v_ref.shape
    ny_cells, size_z = mat.shape[2:]
    half = ny_cells // 2
    group = size_z + GHOST
    hz = half * size_z
    kw = t.shape[2]
    tail = GHOST + own
    gx, gy, gz = (lax.axis_index(a) for a in AXES)
    cx, cy, cz = (lax.axis_size(a) for a in AXES)
    has = {("gx", -1): gx > 0, ("gx", 1): gx < cx - 1, ("gy", -1): gy > 0, ("gy", 1): gy < cy - 1}
    at = {"gx": gx, "gy": gy}
    top = has["gy", 1]
    other = lax.rem(gz + 1, cz)
    barrier = pltpu.get_barrier_semaphore()
    total = 0
    for axis, count in (("gz", cz), ("gy", cy), ("gx", cx)):
        me = lax.axis_index(axis)
        for k in range(1, count):
            pl.semaphore_signal(barrier, inc=1, device_id={axis: lax.rem(me + k, count)},
                                device_id_type=MESH)
        total += count - 1
    for sign in (-1, 1):
        @pl.when(has["gy", sign])
        def _(sign=sign):
            pl.semaphore_signal(barrier, inc=1, device_id={"gy": gy + sign, "gz": other},
                                device_id_type=MESH)
        total = total + jnp.where(has["gy", sign], 1, 0)
    diagonals = [(a, b) for a in (-1, 1) for b in (-1, 1)]

    def both_ways(a, b):
        return jnp.logical_and(has["gx", a], has["gy", b])

    for a, b in diagonals:
        @pl.when(both_ways(a, b))
        def _(a=a, b=b):
            pl.semaphore_signal(barrier, inc=1, device_id={"gx": gx + a, "gy": gy + b},
                                device_id_type=MESH)
        total = total + jnp.where(both_ways(a, b), 1, 0)

    own_m = pltpu.make_async_copy(mat_ref, mat, local.at[0])
    own_m.start()
    step = nx // 4
    own_v = [pltpu.make_async_copy(v_ref.at[n * step:(n + 1) * step],
                                   e.at[1 + n * step:1 + (n + 1) * step, GHOST:tail], local.at[2 + n])
             for n in range(4)]
    for copy in own_v:
        copy.start()
    own_t = pltpu.make_async_copy(t_hbm.at[gz], t, local.at[1])
    own_t.start()

    used = [0]
    sent = []

    def remote(src, dst, device, cond=None, got=None):
        n = used[0]
        used[0] += 1
        copy = pltpu.make_async_remote_copy(src_ref=src, dst_ref=dst, send_sem=send.at[n],
                                            recv_sem=recv.at[n], device_id=device,
                                            device_id_type=MESH)

        def when(test, action):
            if test is None:
                action()
            else:
                pl.when(test)(action)

        sent.append(lambda: when(cond, copy.wait_send))
        return lambda: when(cond, copy.start), lambda: when(got, copy.wait_recv)

    def shift(axis, sign, src, dst):
        return remote(src, dst, {axis: at[axis] + sign}, has[axis, sign], has[axis, -sign])

    def partner(src, dst, cond=None):
        return remote(src, dst, {"gz": other}, cond, cond)

    def zero(cond, ref):
        @pl.when(jnp.logical_not(cond))
        def _():
            ref[...] = jnp.zeros(ref.shape, ref.dtype)

    mid = slice(8, 8 + nx)
    zero(has["gx", -1], e.at[0])
    zero(has["gx", 1], e.at[nx + 1])
    zero(has["gy", -1], m.at[:, 0, mid])
    zero(top, m.at[:, ny_cells + 1, mid])
    zero(has["gx", -1], xf_in.at[1])
    zero(has["gx", 1], xf_in.at[0])
    for at_row in (0, 8 + nx):
        m[:, :, at_row:at_row + 8] = jnp.zeros((2, ny_cells + 2, 8, LANES), f32)
    for n, (a, b) in enumerate(diagonals):
        zero(both_ways(-a, -b), c_in.at[n])
    zero(top, g.at[1:nx + 1])
    zero(jnp.logical_and(top, has["gx", -1]), g.at[0])
    zero(jnp.logical_and(top, has["gx", 1]), g.at[nx + 1])
    zero(top, cz_in)
    m[:, 1:ny_cells + 1, mid] = jnp.zeros((2, ny_cells, nx, LANES), f32)
    own_m.wait()
    for f in range(2):
        for y in range(ny_cells):
            m[f, y + 1, mid, :size_z] = mat[f, :, y, :]
    first_x, last_x = 8, 7 + nx
    c_out[...] = jnp.zeros(c_out.shape, f32)
    for f in range(2):
        xf_out[0, f] = m[f, 1:ny_cells + 1, first_x, :]
        xf_out[1, f] = m[f, 1:ny_cells + 1, last_x, :]
        for n, (a, b) in enumerate(diagonals):
            x, y = first_x if a < 0 else last_x, 1 if b < 0 else ny_cells
            c_out[n, f, 0:1] = m[f, y, x:x + 1]

    pl.semaphore_wait(barrier, total)

    my_down = shift("gy", -1, m.at[:, 1, mid], m.at[:, ny_cells + 1, mid])
    my_up = shift("gy", 1, m.at[:, ny_cells, mid], m.at[:, 0, mid])
    mx_down = shift("gx", -1, xf_out.at[0], xf_in.at[0])
    mx_up = shift("gx", 1, xf_out.at[1], xf_in.at[1])
    corners = [remote(c_out.at[n], c_in.at[n], {"gx": gx + a, "gy": gy + b},
                      both_ways(a, b), both_ways(-a, -b)) for n, (a, b) in enumerate(diagonals)]
    material_copies = [my_down, my_up, mx_down, mx_up] + corners
    for copy in material_copies:
        copy[0]()
    bounds = [(nx - 1, nx), (0, 1), (1, 3), (3, 7), (7, nx - 5), (nx - 5, nx - 3), (nx - 3, nx - 1)]
    y_ghosts = [shift("gy", -1, v_ref.at[a:b, :size_z], g.at[a + 1:b + 1, :size_z]) for a, b in bounds]
    for copy in y_ghosts[:3]:
        copy[0]()
    x_down = shift("gx", -1, v_ref.at[0], e.at[nx + 1, GHOST:tail])
    x_up = shift("gx", 1, v_ref.at[nx - 1], e.at[0, GHOST:tail])

    x_down[0]()
    x_up[0]()

    edge = jnp.where(gz == 0, size_z - 1, 0)
    row = lax.broadcasted_iota(jnp.int32, (GHOST, own), 0)
    col = lax.broadcasted_iota(jnp.int32, (GHOST, own), 1)
    pick = jnp.logical_and(row < ny_cells, col == row * size_z + edge)
    pick = jnp.where(pick, 1.0, 0.0).astype(bf16)

    def take_edge(x):
        zs[x] = jnp.dot(pick, e[x, GHOST:tail], preferred_element_type=f32).astype(bf16)

    z_own = []
    for n in range(4):
        own_v[n].wait()
        low, high = 1 + n * step, 1 + (n + 1) * step
        for x in range(low, high):
            take_edge(x)
        z_own.append([partner(zs.at[low:high], e.at[low:high, :GHOST]),
                      partner(zs.at[low:high], e.at[low:high, tail:])])
        for copy in z_own[n]:
            copy[0]()
    row = lax.broadcasted_iota(jnp.int32, (nx, nx * GHOST), 0)
    col = lax.broadcasted_iota(jnp.int32, (nx, nx * GHOST), 1)
    pick2 = jnp.where(col == row * GHOST, 1.0, 0.0).astype(bf16)
    cz_out[...] = jnp.dot(pick2, zs[1:nx + 1].reshape(nx * GHOST, columns),
                          preferred_element_type=f32).astype(bf16)
    corner = remote(cz_out, cz_in, {"gy": gy - 1, "gz": other}, has["gy", -1], top)
    corner[0]()
    for copy in y_ghosts[3:]:
        copy[0]()
    own_t.wait()

    ring_size = pp.shape[0]

    def ring(x):
        return pp.at[x % ring_size]

    def taps_of(x, dst, *more):
        first = jnp.dot(t[0], e[x + 1, :kw], preferred_element_type=f32)
        second = jnp.dot(t[1], e[x + 1, tail + GHOST - kw:], preferred_element_type=f32)
        for ref in (dst,) + more:
            ref[:2 * hz] = first
            ref[2 * hz:] = second

    acc[...] = jnp.zeros_like(acc)
    def arrived(n):
        for copy in z_own[n]:
            copy[1]()

    arrived(0)
    taps_of(0, ring(0), ps0)
    taps_of(1, ring(1), ps1)
    for x in range(2, step):
        taps_of(x, ring(x))
    for copy in material_copies:
        copy[1]()
    for f in range(2):
        for y in range(ny_cells):
            m[f, y + 1, last_x + 1:last_x + 2] = xf_in[0, f, y:y + 1]
            m[f, y + 1, first_x - 1:first_x] = xf_in[1, f, y:y + 1]
        for n, (a, b) in enumerate(diagonals):
            x, y = last_x + 1 if a < 0 else first_x - 1, ny_cells + 1 if b < 0 else 0
            m[f, y, x:x + 1] = c_in[n, f, 0:1]
    mz_copy = partner(m, mz)
    mz_copy[0]()
    arrived(1)
    for x in range(step, step + 2):
        taps_of(x, ring(x))
    for n in range(2, 4):
        arrived(n)
    ready = ring_size - 1
    for x in range(step + 2, ready):
        taps_of(x, ring(x))
    mz_copy[1]()

    lanes = lax.broadcasted_iota(jnp.int32, (m.shape[2], LANES), 1)
    turn = jnp.where(gz == 0, size_z - 1, LANES - size_z + 1)

    def z_sum(y):
        k = m[0, y]
        ghost = jnp.where(lanes == edge, pltpu.roll(mz[0, y], turn, 1), 0.0)
        return pltpu.roll(k, 1, 1) + 2.0 * k + pltpu.roll(k, LANES - 1, 1) + ghost

    sums = [z_sum(y) for y in range(ny_cells + 2)]
    for y in range(ny_cells):
        fy[y] = sums[y] + 2.0 * sums[y + 1] + sums[y + 2]
        field = fy[y, 7:7 + nx] + 2.0 * fy[y, 8:8 + nx] + fy[y, 9:9 + nx]
        kappa = m[0, y + 1, mid]
        rho = m[1, y + 1, mid]
        both = jnp.concatenate([2.0 * kappa + field * (1.0 / 32.0), kappa * (1.0 / 16.0),
                                rho * (1.0 / 216.0)], 0)
        cols[y, :, :3 * nx] = both.T[:size_z]

    dims = (((0,), (0,)), ((), ()))

    def column(x, y, c):
        return jnp.broadcast_to(cols[y, :, c * nx + x:c * nx + x + 1], (size_z, LANES))

    def values(xs, planes, dst, base=0):
        for y in range(ny_cells):
            h, yy = divmod(y, half)
            sr = slice(2 * hz * h + size_z * yy, 2 * hz * h + size_z * (yy + 1))
            mr = slice(sr.start + hz, sr.stop + hz)
            coef = [[column(x, y, c) for c in range(3)] for x in xs]
            for at_lane in range(0, columns, LANES):
                ll = slice(at_lane, at_lane + LANES)
                p = [ref[sr, ll] for ref in planes]
                q = [ref[mr, ll] for ref in planes]
                for k, x in enumerate(xs):
                    d, kq, rq = coef[k]
                    rr = slice(base + k * own + size_z * y, base + k * own + size_z * (y + 1))
                    v = e[x + 1, GHOST + size_z * y:GHOST + size_z * (y + 1), ll].astype(f32)
                    s = p[k] + p[k + 2] + 2.0 * p[k + 1]
                    w = q[k] + q[k + 2] + 4.0 * q[k + 1]
                    dst[rr, ll] = (d * v - kq * s).astype(bf16)
                    dst[rr, slice(columns + at_lane, columns + at_lane + LANES)] = (rq * w).astype(bf16)

    def gram(first, second, src):
        v = jnp.concatenate([e[first + 1, GHOST:tail], e[second + 1, GHOST:tail]], 0)
        acc[...] += lax.dot_general(v, src[...], dims, preferred_element_type=f32)

    def relay(sign, src, dst):
        return remote(g.at[src, :size_z], g.at[dst, :size_z], {"gx": gx + sign},
                      jnp.logical_and(top, has["gx", sign]), jnp.logical_and(top, has["gx", -sign]))

    relays = [relay(-1, 1, nx + 1), relay(1, nx, 0)]
    z_ghosts = [partner(zs.at[x], e.at[x, at_row:at_row + GHOST])
                for x in (0, nx + 1) for at_row in (0, tail)]
    zrow = pl.multiple_of(jnp.where(gz == 0, size_z - GHOST, 0), GHOST)
    z_relays = [partner(g.at[j, pl.ds(zrow, GHOST)], g.at[j, size_z:], top) for j in (0, nx + 1)]

    reach = jnp.where(gz == 0, size_z, GHOST)
    mine = lanes < size_z

    def ghost_columns(f, factor):
        k = m[f, ny_cells + 1]
        return jnp.where(mine, k, pltpu.roll(mz[f, ny_cells + 1], reach, 1)) * factor

    def prepare_ghosts():
        both = jnp.concatenate([ghost_columns(0, 1.0 / 16.0), ghost_columns(1, 1.0 / 216.0)], 0)
        ghost_cols = both.T[:group]
        for f in range(2):
            for j in range(nx + 2):
                n = f * m.shape[2] + 7 + j
                gc[f, j] = jnp.broadcast_to(ghost_cols[:, n:n + 1], (group, LANES))
        for x in range(nx):
            one = cz_in[x:x + 1].astype(f32)
            g[x + 1, size_z:] = jnp.broadcast_to(one, (GHOST, columns)).astype(bf16)

    two_z = 2 * size_z

    def weigh(j):
        for at_lane in range(0, columns, LANES):
            ll = slice(at_lane, at_lane + LANES)
            v = g[j, :, ll].astype(f32)
            gk[j, :, ll] = (v * gc[0, j]).astype(bf16)
            gr[j, :, ll] = (v * gc[1, j]).astype(bf16)

    def late(x, side):
        taps = t[2, side * two_z:(side + 1) * two_z, :4 * group]
        weighed = (gk, gr)[side]
        coef = [column(x + o, ny_cells - 1, 1 + side) for o in range(2)]
        for at_lane in range(0, columns, 2 * LANES):
            ll = slice(at_lane, at_lane + 2 * LANES)
            plain = jnp.dot(taps, g[x:x + 4, :, ll].reshape(4 * group, 2 * LANES),
                            preferred_element_type=f32)
            heavy = jnp.dot(taps, weighed[x:x + 4, :, ll].reshape(4 * group, 2 * LANES),
                            preferred_element_type=f32)
            for o in range(2):
                rr = slice(o * size_z, (o + 1) * size_z)
                c = jnp.concatenate([coef[o]] * 2, 1)
                if side == 0:
                    value = (-c) * plain[rr] - heavy[rr]
                else:
                    value = c * plain[rr] + heavy[rr]
                yl[side, x + o, :, ll] = value.astype(bf16)

    def late_gram(first, stop, side):
        v = jnp.concatenate([e[x + 1, tail - size_z:tail] for x in range(first, stop)], 0)
        y = yl[side, first:stop].reshape((stop - first) * size_z, columns)
        ll = slice(side * columns, (side + 1) * columns)
        acc[:, ll] += lax.dot_general(v, y, dims, preferred_element_type=f32)

    def stage(n):
        if n == 3:
            for copy in y_ghosts[:2]:
                copy[1]()
            for copy in relays:
                copy[0]()
        elif n == 5:
            x_down[1]()
            x_up[1]()
            take_edge(0)
            take_edge(nx + 1)
            for copy in z_ghosts:
                copy[0]()
            for copy in relays:
                copy[1]()
            for copy in z_relays:
                copy[0]()
        elif n == 6:
            for copy in z_ghosts:
                copy[1]()
            corner[1]()
        elif n == 7:
            for copy in z_relays:
                copy[1]()
            for copy in y_ghosts[2:5]:
                copy[1]()

    pairs = [(x, x + 1) for x in range(1, nx - 1, 2)] + [(nx - 1, 0)]
    previous = None
    for n, pair in enumerate(pairs):
        stage(n)
        y_now = (ya, yb)[n % 2]
        if pair[1]:
            values(pair, [ring(x) for x in range(pair[0] - 1, pair[1] + 2)], y_now)
        else:
            values((nx - 1,), [ring(nx - 2), ring(nx - 1), ring(nx)], y_now)
            values((0,), [ring(nx + 1), ps0, ps1], y_now, own)
        for x in (ready + 2 * n, ready + 2 * n + 1):
            if x < nx:
                taps_of(x, ring(x))
        if n == 6:
            taps_of(nx, ring(nx))
            taps_of(-1, ring(nx + 1))
        if n == 6:
            prepare_ghosts()
        if previous is not None:
            gram(*previous)
        previous = pair + (y_now,)
    soon = nx - 6
    for j in list(range(soon + 2)) + [nx, nx + 1]:
        weigh(j)
    for x in range(0, soon, 2):
        late(x, 0)
    gram(*previous)
    late_gram(0, soon, 0)
    y_ghosts[5][1]()
    for j in range(soon + 2, soon + 4):
        weigh(j)
    late(soon, 0)
    y_ghosts[6][1]()
    for j in range(soon + 4, nx):
        weigh(j)

    def finish(side):
        for x in range(soon + 2, nx, 2):
            late(x, side)
        late_gram(soon, nx, side)

    rows = out_ref.shape[0]

    def symmetric(side):
        ll = slice(side * columns, (side + 1) * columns)
        a = acc[:, ll]
        a = (a + a.T) * scale
        for n in range(columns // rows):
            i, rest = divmod(n, cy * cz)
            j, k = divmod(rest, cz)
            part[i, j, k, :, ll] = a[n * rows:(n + 1) * rows]

    def everywhere(axis, piece, landing):
        count = lax.axis_size(axis)
        me = lax.axis_index(axis)
        n = used[0]
        used[0] += 1

        def copy(src, dst, peer):
            return pltpu.make_async_remote_copy(src_ref=src, dst_ref=dst, send_sem=send.at[n],
                                                recv_sem=recv.at[n], device_id={axis: peer},
                                                device_id_type=MESH)

        for k in range(1, count):
            peer = lax.rem(me + k, count)
            copy(piece(peer), landing.at[k - 1], peer).start()
        whole = copy(landing, landing, lax.rem(me + 1, count))
        sent.append(whole.wait_send)
        return whole.wait_recv

    def collect(arrive, held, landing):
        arrive()
        for k in range(landing.shape[0]):
            held = held + landing[k]
        return held

    flights = [None] * len(chunks)

    def leave(n):
        lo, hi, by = chunks[n]
        flights[n] = everywhere("gz", lambda p: part.at[:, :, p, :, lo:hi], buffers[n][0])

    def first_round(n):
        lo, hi, by = chunks[n]
        rz, s1, r1, s2, r2 = buffers[n]
        s1[...] = collect(flights[n], part[:, :, gz, :, lo:hi], rz)
        if by == "gy":
            flights[n] = everywhere("gy", lambda p: s1.at[:, p], r1)
        else:
            flights[n] = everywhere("gx", lambda p: s1.at[p], r1)

    halves = [[n for n, c in enumerate(chunks) if c[0] // columns == side] for side in range(2)]
    finish(0)
    symmetric(0)
    for n in halves[0]:
        leave(n)
    for x in range(0, soon + 2, 2):
        late(x, 1)
    late_gram(0, soon, 1)
    for n in halves[0]:
        first_round(n)
    finish(1)
    symmetric(1)
    for n in halves[1]:
        leave(n)
    for n in halves[1]:
        first_round(n)
    for n, (lo, hi, by) in enumerate(chunks):
        rz, s1, r1, s2, r2 = buffers[n]
        mine_now = s1[:, gy] if by == "gy" else s1[gx]
        s2[...] = collect(flights[n], mine_now, r1)
        flights[n] = everywhere("gx" if by == "gy" else "gy", lambda p, s2=s2: s2.at[p], r2)
    for n, (lo, hi, by) in enumerate(chunks):
        rz, s1, r1, s2, r2 = buffers[n]
        out_ref[:, lo:hi] = collect(flights[n], s2[gx] if by == "gy" else s2[gy], r2)
    for done in sent:
        done()


def per_device(eigvecs, material):
    size_x, size_y, size_z, columns = eigvecs.shape
    nx, ny, nz = (lax.axis_size(a) for a in ("gx", "gy", "gz"))
    total_cells = size_x * size_y * size_z * nx * ny * nz
    own = size_y * size_z
    tail = own + 2 * GHOST
    group = size_z + GHOST
    rows = columns // (nx * ny * nz)
    wide = 2 * columns
    matrices = jnp.asarray(tap_matrices(size_y, size_z), jnp.bfloat16)
    parts = ((2, "gy"), (2, "gx"), (2, "gy"), (1, "gy"), (1, "gy"))
    unit = wide // 8
    chunks, lo = [], 0
    for width, by in parts:
        chunks.append((lo, lo + width * unit, by))
        lo += width * unit
    f32, bf16 = jnp.float32, jnp.bfloat16
    dma = pltpu.SemaphoreType.DMA
    vmem = pl.BlockSpec(memory_space=pltpu.VMEM)
    anywhere = pl.BlockSpec(memory_space=pl.ANY)
    copies = 35 + len(chunks) * 3
    plane = ((2 * own, columns), f32)
    face, corner = ((2, 2, size_y, LANES), f32), ((4, 2, 8, LANES), f32)
    scratch = [
        (material.shape, f32), face, face, corner, corner,
        ((size_x + 2, tail, columns), bf16),
        ((12, 2 * own, columns), f32), plane, plane,
        ((2 * own, wide), bf16), ((2 * own, wide), bf16),
        ((columns, wide), f32),
        (matrices.shape[1:], bf16),
        ((size_x + 2, GHOST, columns), bf16),
        ((size_x, columns), bf16),
        ((size_x, columns), bf16),
        ((2, size_y + 2, size_x + 16, LANES), f32),
        ((2, size_y + 2, size_x + 16, LANES), f32),
        ((size_y, size_x + 16, LANES), f32),
        ((size_y, size_z, LANES), f32),
        ((2, size_x + 2, group, LANES), f32),
        ((size_x + 2, group, columns), bf16),
        ((size_x + 2, group, columns), bf16),
        ((size_x + 2, group, columns), bf16),
        ((2, size_x, size_z, columns), bf16),
        ((nx, ny, nz, rows, wide), f32),
    ]
    for low, high, by in chunks:
        w = high - low
        n1, n2 = (ny, nx) if by == "gy" else (nx, ny)
        scratch += [((nz - 1, nx, ny, rows, w), f32), ((nx, ny, rows, w), f32),
                    ((n1 - 1, n2, rows, w), f32), ((n2, rows, w), f32), ((n2 - 1, rows, w), f32)]
    out = pl.pallas_call(
        functools.partial(kernel, 0.5 / total_cells, tuple(chunks)),
        out_shape=pltpu.VMEM((rows, wide), f32),
        in_specs=[anywhere] * 3,
        out_specs=vmem,
        scratch_shapes=[pltpu.VMEM(*s) for s in scratch] + [dma((6,)), dma((copies,)), dma((copies,))],
        compiler_params=pltpu.CompilerParams(
            vmem_limit_bytes=63 * 1024 * 1024, collective_id=0, has_side_effects=True),
    )(eigvecs.reshape(size_x, own, columns), material, matrices)
    return out[:, :columns], out[:, columns:]


def solution(mesh):
    return jax.shard_map(
        per_device,
        mesh=mesh,
        in_specs=(P("gx", "gy", "gz", None), P(None, "gx", "gy", "gz")),
        out_specs=(P(("gx", "gy", "gz"), None), P(("gx", "gy", "gz"), None)),
        check_vma=False,
    )
```
